768 devices in a mesh: enc: 12 (over z), grp: 64 (over x, y, core).
Axes of the slice: x: 4, y: 8, z: 12, core: 2. Of those that a mesh axis runs over, the one named last changes fastest.
Arguments:
- patch_feats: bfloat16 [12, 4096, 8, 1152], P('enc', 'grp'), may hold values from -6 to 6
- windows: int32 [12, 4096, 3, 4], P('enc', 'grp'), may hold values from 0 to 7
- counts: int32 [12, 4096], P('enc', 'grp'), may hold values from 1 to 3
- owners: int32 [12, 4096], P('enc', 'grp'), may hold values from 0 to 63, as said below
- norm_gain: float32 [1152], replicated, may hold values from 0.1 to 1.9
- norm_bias: float32 [1152], replicated, may hold values from -1.8 to 1.8
- proj_weight: bfloat16 [1152, 4096], replicated, may hold values from -0.1875 to 0.1875
- proj_bias: float32 [4096], replicated, may hold values from -3 to 3
Outputs:
- projected: bfloat16 [12, 12288, 4096], P('enc', 'grp')
The draws below stay inside these ranges and needn't reach their ends.
Inputs may be any that keep to these rules, and one draw needn't show every extreme that they name: `owners`: within each frame index, each aligned block of 64 clips (the clips of one device) names any section-0 rank at most 1 times, and some rank exactly 1 times.
All inputs are finite; a program needn't handle non-finite values.
Results may differ from the reference program's by a relative error of at most 0.0051.
Values may be sent and summed in bfloat16 or wider, within the bound.
A program may use at most 32 MiB of HBM per device.

```python
import jax
import jax.numpy as jnp
from jax import lax

D = 1152
DL = 4096
SAMP_DEV = 64
PSAMP = 8
SEG = 3
WIN = 4
CLIPS = 4096
MOST = 1
OWN_ROWS = 192
N_ENC = 12
N_GRP = 64


def draw_owners(key, part):
    block_keys = jax.random.split(jax.random.fold_in(key, 17), N_ENC * N_GRP)

    def one_block(block_key):
        first_key, second_key = jax.random.split(block_key)
        ranking = jax.random.permutation(first_key, N_GRP)
        repeated = jnp.tile(ranking, MOST)[:SAMP_DEV]
        shuffle = jax.random.permutation(second_key, SAMP_DEV)
        return repeated[shuffle]
    blocks = jax.vmap(one_block)(block_keys)
    return blocks.reshape(N_ENC, N_GRP * SAMP_DEV).astype(jnp.int32)


def with_ends(result, stream_key, low, largest):
    extent = result.shape
    spot = [jax.random.randint(jax.random.fold_in(stream_key, axis), (), 0, extent[axis]) for axis in range(len(extent))]
    result = result.at[tuple(spot)].set(low)
    longest = extent.index(max(extent))
    spot[longest] = (spot[longest] + 1) % extent[longest]
    return result.at[tuple(spot)].set(largest)


def levels(stream_key, extent, cuts, smallest, top_value):
    loudness, own = 1.0, jax.random.fold_in(stream_key, 6)
    for axis_at, blocks in cuts:
        heights = jnp.exp(jax.random.uniform(jax.random.fold_in(own, axis_at), (blocks,), jnp.float32, smallest / len(cuts), top_value / len(cuts)))
        loudness = loudness * jnp.repeat(heights, extent[axis_at] // blocks).reshape([-1 if axis == axis_at else 1 for axis in range(len(extent))])
    return loudness


def gaussian(key, dims, scale, bound, cuts=(), dtype=jnp.bfloat16):
    drawn = scale * jax.random.normal(key, dims, jnp.float32)
    if cuts:
        drawn = drawn * levels(key, dims, cuts, -0.22, 0.18)
    return jnp.clip(drawn, -bound, bound).astype(dtype)


def setup_inputs(seed: int = 0) -> dict:
    seeds = jax.random.split(jax.random.key(seed), 9)
    patch_feats = gaussian(seeds[0], (N_ENC, CLIPS, PSAMP, D), 1.0, 6.0, ((0, 12), (1, 64)))
    windows = with_ends(jax.random.randint(seeds[1], (N_ENC, CLIPS, SEG, WIN), 0, PSAMP), jax.random.fold_in(seeds[1], 1), 0, PSAMP - 1).astype(jnp.int32)
    counts = with_ends(jax.random.randint(seeds[2], (N_ENC, CLIPS), 1, SEG + 1), jax.random.fold_in(seeds[2], 1), 1, SEG).astype(jnp.int32)
    owners = draw_owners(jax.random.fold_in(seeds[8], 71), 0)
    norm_gain = jnp.clip(1.0 + 0.18 * jax.random.normal(seeds[4], (D,), jnp.float32), 0.1, 1.9)
    norm_bias = gaussian(seeds[5], (D,), 0.3, 1.8, (), jnp.float32)
    proj_weight = gaussian(seeds[6], (D, DL), D ** -0.5, 0.1875)
    proj_bias = gaussian(seeds[7], (DL,), 0.5, 3.0, (), jnp.float32)
    return dict(patch_feats=patch_feats, windows=windows, counts=counts, owners=owners, norm_gain=norm_gain, norm_bias=norm_bias, proj_weight=proj_weight, proj_bias=proj_bias)


def pool_frame(frame_feats, frame_windows, norm_gain, norm_bias):
    values = frame_feats.astype(jnp.float32)
    average = lax.optimization_barrier(jnp.mean(values, axis=-1, keepdims=True))
    spread = lax.optimization_barrier(jnp.mean((values - average) ** 2, axis=-1, keepdims=True))
    normed = (values - average) * lax.rsqrt(spread + 1e-06) * norm_gain + norm_bias
    patch_ids = jnp.arange(PSAMP).astype(jnp.int32)
    selector = lax.optimization_barrier(jnp.sum((frame_windows[..., None] == patch_ids).astype(jnp.float32), axis=2)) / WIN
    pooled = jnp.einsum('cst,ctd->csd', selector, normed, precision=lax.Precision.HIGHEST)
    return pooled.astype(jnp.bfloat16)

def reference(patch_feats, windows, counts, owners, norm_gain, norm_bias, proj_weight, proj_bias):
    pooled = lax.map(lambda pair: pool_frame(pair[0], pair[1], norm_gain, norm_bias), (patch_feats, windows))
    following = jnp.concatenate([pooled[1:], pooled[-1:]], axis=0)
    merged = ((pooled.astype(jnp.float32) + following.astype(jnp.float32)) * 0.5).astype(jnp.bfloat16)
    rank_ids = jnp.arange(N_GRP).astype(jnp.int32)
    slot_index = jnp.arange(SEG).astype(jnp.int32)

    def place(triple):
        merged_f, counts_f, owners_f = triple
        matches = (owners_f[:, None] == rank_ids[None, :]).astype(jnp.int32)
        weighted = matches * counts_f[:, None]
        earlier = jnp.cumsum(weighted, axis=0) - weighted
        start = lax.optimization_barrier(jnp.sum(earlier * matches, axis=1)).astype(jnp.int32)
        row_index = owners_f[:, None] * OWN_ROWS + start[:, None] + slot_index[None, :]
        row_index = jnp.where(slot_index[None, :] < counts_f[:, None], row_index, N_GRP * OWN_ROWS).astype(jnp.int32)
        flat_rows = merged_f.reshape(-1, D)
        product = jnp.dot(flat_rows, proj_weight, preferred_element_type=jnp.float32) + proj_bias
        rounded = product.astype(jnp.bfloat16)
        placed = jnp.zeros((N_GRP * OWN_ROWS, DL), jnp.bfloat16)
        return placed.at[row_index.reshape(-1)].set(rounded, mode='drop')
    return lax.map(place, (merged, counts, owners))
```

```python
import jax
import jax.numpy as jnp
from jax import lax
from jax.experimental import pallas as pl
from jax.experimental.pallas import tpu as pltpu
from jax.sharding import PartitionSpec as P

MESH = pl.DeviceIdType.MESH
F32 = jnp.float32
BF16 = jnp.bfloat16
LANES = 128
WIDTH = 1152
OUT_WIDTH = 4096
CLIPS = 64
PATCHES = 8
TOKENS = 3
RANKS = 64
ROWS = CLIPS * TOKENS
TILES = WIDTH // LANES
UNITS = ((0, 5), (1, 6), (2, 7), (3, 8), (4,))
PLACE = {tile: i for i, tile in enumerate(t for unit in UNITS for t in unit)}
ORDER = (4, 0, 1, 2, 3)
SLOT_TILES = 14


def iota(shape, dim):
    return lax.broadcasted_iota(jnp.int32, shape, dim)


def peer_of(step, me):
    x, y, core = me // 16, (me // 2) % 8, me % 2
    dx, dy, dcore = step // 16, (step // 2) % 8, step % 2
    return ((x + dx) % 4) * 16 + ((y + dy) % 8) * 2 + (core + dcore) % 2


def unit_tiles(unit):
    return 3 * unit, 3 if unit < 4 else 2


def exchange(
    feats_hbm, win_ref, counts_ref, owners_ref, gain_ref, bias_ref,
    packed_ref, live_ref,
    feats, stats, mine, theirs, outgoing, arrived,
    feat_sem, z_send, z_recv, x_send, x_recv, own_sem,
):
    me = lax.axis_index("grp")
    frame = lax.axis_index("enc")
    last = lax.axis_size("enc") - 1
    fetch = pltpu.make_async_copy(feats_hbm, feats, feat_sem)
    fetch.start()

    barrier = pltpu.get_barrier_semaphore()

    def greet(step, carry):
        pl.semaphore_signal(
            barrier, inc=1, device_id={"grp": peer_of(RANKS - step, me)}, device_id_type=MESH
        )
        return carry

    lax.fori_loop(1, RANKS, greet, 0)
    before = jnp.maximum(frame - 1, 0)
    after = jnp.minimum(frame + 1, last)

    @pl.when(frame > 0)
    def _():
        pl.semaphore_signal(barrier, inc=1, device_id={"enc": before}, device_id_type=MESH)

    @pl.when(frame < last)
    def _():
        pl.semaphore_signal(barrier, inc=1, device_id={"enc": after}, device_id_type=MESH)

    fetch.wait()
    group = 32

    def statistics(i, carry):
        at = pl.ds(pl.multiple_of(i * group, group), group)
        values = feats[at, :].astype(F32)
        mean = jnp.sum(values, axis=1, keepdims=True) * (1.0 / WIDTH)
        centred = values - mean
        var = jnp.sum(centred * centred, axis=1, keepdims=True) * (1.0 / WIDTH)
        stats[0, at, :] = jnp.broadcast_to(mean, (group, LANES))
        stats[1, at, :] = jnp.broadcast_to(lax.rsqrt(var + 1e-6), (group, LANES))
        return carry

    lax.fori_loop(0, CLIPS * PATCHES // group, statistics, 0)
    diagonal = iota((LANES, LANES), 0) == iota((LANES, LANES), 1)

    def as_row(which, start):
        column = stats[which, pl.ds(start, LANES), :]
        return jnp.sum(jnp.where(diagonal, column, 0.0), axis=0, keepdims=True)

    half = CLIPS // 2
    depth = half * PATCHES
    clip_diagonal = iota((CLIPS, CLIPS), 0) == iota((CLIPS, CLIPS), 1)

    def pick_column(token, w):
        row = win_ref[token, w : w + 1, :]
        return jnp.sum(jnp.where(clip_diagonal, row, 0), axis=1, keepdims=True)

    picked = [
        [pick_column(token, w) + PATCHES * (iota((CLIPS, 1), 0) % half) for w in range(4)]
        for token in range(TOKENS)
    ]
    for block in range(2):
        start = block * depth
        mean_row = jnp.concatenate([as_row(0, start), as_row(0, start + LANES)], axis=1)
        rstd_row = jnp.concatenate([as_row(1, start), as_row(1, start + LANES)], axis=1)
        parts = []
        for token in range(TOKENS):
            lanes = iota((half, depth), 1)
            weight = jnp.zeros((half, depth), F32)
            for w in range(4):
                picks = picked[token][w][block * half : (block + 1) * half]
                weight += jnp.where(picks == lanes, 0.25, 0.0)
            parts.append(weight)
        scaled = jnp.concatenate(parts, axis=0) * rstd_row
        shift = jnp.sum(scaled * mean_row, axis=1, keepdims=True)
        high = scaled.astype(BF16)
        rest = scaled - high.astype(F32)
        middle = rest.astype(BF16)
        low = (rest - middle.astype(F32)).astype(BF16)
        selector = jnp.concatenate([high, middle, low], axis=0)
        height = TOKENS * half
        for column in range(0, WIDTH, 2 * LANES):
            wide = min(2 * LANES, WIDTH - column)
            product = jnp.dot(
                selector, feats[pl.ds(start, depth), pl.ds(column, wide)],
                preferred_element_type=F32,
            )
            total = product[:height] + product[height : 2 * height] + product[2 * height :]
            pooled = (total - shift) * gain_ref[:, pl.ds(column, wide)]
            pooled = (pooled + bias_ref[:, pl.ds(column, wide)]).astype(BF16)
            for i in range(wide // LANES):
                place = PLACE[column // LANES + i]
                for token in range(TOKENS):
                    mine[place, pl.ds(token * CLIPS + block * half, half), :] = pooled[
                        token * half : (token + 1) * half, i * LANES : (i + 1) * LANES
                    ]

    @pl.when(frame == last)
    def _():
        theirs[...] = mine[...]

    owner_row = owners_ref[...]
    count_row = counts_ref[...].astype(F32)
    rank = iota((2 * RANKS, CLIPS), 0) // 2
    odd = iota((2 * RANKS, CLIPS), 0) % 2
    owned = jnp.where(owner_row == rank, 1.0, 0.0)
    even_rows = jnp.where(odd == 0, owned, 0.0)
    odd_rows = jnp.where(odd == 1, owned, 0.0)
    place_matrix = jnp.concatenate([even_rows, odd_rows], axis=1).astype(BF16)
    count_column = jnp.sum(odd_rows * count_row, axis=1, keepdims=True)

    neighbours = jnp.minimum(frame, 1) + jnp.minimum(last - frame, 1)
    pl.semaphore_wait(barrier, RANKS - 1 + neighbours)

    def shift_copy(unit):
        at = pl.ds(2 * unit, len(UNITS[unit]))
        return pltpu.make_async_remote_copy(
            mine.at[at], theirs.at[at], z_send.at[unit], z_recv.at[unit],
            device_id={"enc": before}, device_id_type=MESH,
        )

    @pl.when(frame > 0)
    def _():
        for unit in ORDER:
            shift_copy(unit).start()

    def own_copy(unit):
        at = pl.ds(*unit_tiles(unit))
        return pltpu.make_async_copy(
            outgoing.at[at, me], arrived.at[at, me], own_sem.at[unit]
        )

    for unit in ORDER:
        @pl.when(frame < last)
        def _():
            shift_copy(unit).wait_recv()

        merged = []
        for tile in UNITS[unit]:
            place = PLACE[tile]
            merged.append(
                ((mine[place].astype(F32) + theirs[place].astype(F32)) * 0.5).astype(BF16)
            )
        first, tiles = unit_tiles(unit)
        for i, block in enumerate(merged):
            spread = jnp.dot(place_matrix, block[: 2 * CLIPS], preferred_element_type=F32)
            outgoing[first + i] = spread.astype(BF16).reshape(RANKS, 2, LANES)
        if unit < 4:
            third = jnp.concatenate([block[2 * CLIPS :] for block in merged], axis=0)
            spread = jnp.dot(place_matrix, third, preferred_element_type=F32)
        else:
            spread = jnp.dot(
                even_rows.astype(BF16), merged[0][2 * CLIPS :], preferred_element_type=F32
            )
            spread = spread + count_column
        outgoing[first + tiles - 1] = spread.astype(BF16).reshape(RANKS, 2, LANES)
        own_copy(unit).start()

        def send(step, carry):
            peer = peer_of(RANKS - step, me)
            at = pl.ds(first, tiles)
            pltpu.make_async_remote_copy(
                outgoing.at[at, peer], arrived.at[at, me], x_send.at[unit], x_recv.at[unit],
                device_id={"grp": peer}, device_id_type=MESH,
            ).start()
            return carry

        lax.fori_loop(1, RANKS, send, 0)

    def arrival(unit, sem):
        at = pl.ds(*unit_tiles(unit))
        everyone = pl.ds(0, RANKS - 1)
        return pltpu.make_async_copy(
            outgoing.at[at, everyone], arrived.at[at, everyone], sem.at[unit]
        )

    for unit in ORDER:
        own_copy(unit).wait()
        arrival(unit, x_recv).wait()
        first, tiles = unit_tiles(unit)
        block = [arrived[first + i].reshape(2 * RANKS, LANES) for i in range(tiles)]
        if unit == 4:
            across = iota((2 * RANKS, 2 * RANKS), 1) // 2
            down = iota((2 * RANKS, 2 * RANKS), 0) // 2
            marked = iota((2 * RANKS, 2 * RANKS), 0) % 2 == 1
            earlier = jnp.where(marked & (down < across), 1.0, 0.0)
            same = jnp.where(marked & (down == across), 1.0, 0.0)
            table = jnp.concatenate([earlier, same], axis=1).astype(BF16)
            found = lax.dot_general(
                block[1], table, (((0,), (0,)), ((), ())), preferred_element_type=F32
            )
            opening = found[:1, : 2 * RANKS].astype(jnp.int32)
            count = found[:1, 2 * RANKS :].astype(jnp.int32)
            row = iota((ROWS, 2 * RANKS), 0)
            token = iota((ROWS, 2 * RANKS), 1) % 2
            pair = (row == opening + token) & (token < count)
            third = (row == opening + 2) & (count == 3)
            pair = jnp.where(pair, 1.0, 0.0)
            third_even = jnp.where(third & (token == 0), 1.0, 0.0)
            third_odd = jnp.where(third & (token == 1), 1.0, 0.0)
            live = jnp.sum(pair + third_even, axis=1, keepdims=True)
            live_ref[...] = jnp.broadcast_to(live, (ROWS, LANES))
            pack = (
                jnp.concatenate([pair, third_even], axis=1).astype(BF16),
                jnp.concatenate([pair, third_odd], axis=1).astype(BF16),
            )
        for i, tile in enumerate(UNITS[unit]):
            both = jnp.concatenate([block[i], block[tiles - 1]], axis=0)
            packed = jnp.dot(pack[i], both, preferred_element_type=F32).astype(BF16)
            packed_ref[:, tile * LANES : (tile + 1) * LANES] = packed

    for unit in ORDER:
        arrival(unit, x_send).wait()

    @pl.when(frame > 0)
    def _():
        for unit in ORDER:
            shift_copy(unit).wait_send()


def project(packed_ref, live_ref, weight_ref, bias_ref, result_ref, staged, sems):
    columns = staged.shape[2]
    shown = live_ref[:, :1] > 0.5

    def copy(n):
        at = pl.ds(n * columns, columns)
        return pltpu.make_async_copy(staged.at[n], result_ref.at[:, at], sems.at[n])

    for n in range(OUT_WIDTH // columns):
        at = pl.ds(n * columns, columns)
        product = jnp.dot(packed_ref[...], weight_ref[:, at], preferred_element_type=F32)
        staged[n] = jnp.where(shown, product + bias_ref[:, at], 0.0).astype(BF16)
        copy(n).start()
    for n in range(OUT_WIDTH // columns):
        copy(n).wait()


def shards(patch_feats, windows, counts, owners, norm_gain, norm_bias, proj_weight, proj_bias):
    vmem = pl.BlockSpec(memory_space=pltpu.VMEM)
    units = len(UNITS)
    packed, live = pl.pallas_call(
        exchange,
        name="exchange",
        out_shape=(
            jax.ShapeDtypeStruct((ROWS, WIDTH), BF16),
            jax.ShapeDtypeStruct((ROWS, LANES), F32),
        ),
        in_specs=[pl.BlockSpec(memory_space=pltpu.HBM)] + [vmem] * 5,
        out_specs=(vmem, vmem),
        scratch_shapes=[
            pltpu.VMEM((CLIPS * PATCHES, WIDTH), BF16),
            pltpu.VMEM((2, CLIPS * PATCHES, LANES), F32),
            pltpu.VMEM((TILES, ROWS, LANES), BF16),
            pltpu.VMEM((TILES, ROWS, LANES), BF16),
            pltpu.VMEM((SLOT_TILES, RANKS, 2, LANES), BF16),
            pltpu.VMEM((SLOT_TILES, RANKS, 2, LANES), BF16),
            pltpu.SemaphoreType.DMA,
        ] + [pltpu.SemaphoreType.DMA((units,))] * 5,
        compiler_params=pltpu.CompilerParams(
            collective_id=0, has_side_effects=True, vmem_limit_bytes=24 << 20
        ),
        cost_estimate=pl.CostEstimate(
            flops=60_000_000_000, bytes_accessed=4_000_000, transcendentals=0
        ),
    )(
        patch_feats.reshape(CLIPS * PATCHES, WIDTH), windows[0].transpose(1, 2, 0), counts, owners,
        norm_gain.reshape(1, WIDTH), norm_bias.reshape(1, WIDTH),
    )
    step = 512
    result = pl.pallas_call(
        project,
        name="project",
        out_shape=jax.ShapeDtypeStruct((ROWS, OUT_WIDTH), BF16),
        in_specs=[vmem] * 4,
        out_specs=pl.BlockSpec(memory_space=pltpu.HBM),
        scratch_shapes=[
            pltpu.VMEM((OUT_WIDTH // step, ROWS, step), BF16),
            pltpu.SemaphoreType.DMA((OUT_WIDTH // step,)),
        ],
        compiler_params=pltpu.CompilerParams(vmem_limit_bytes=24 << 20),
        cost_estimate=pl.CostEstimate(
            flops=2 * ROWS * WIDTH * OUT_WIDTH, bytes_accessed=12_000_000, transcendentals=0
        ),
    )(packed, live, proj_weight, proj_bias.reshape(1, OUT_WIDTH))
    return result[None]


def solution(mesh):
    placed = (
        P("enc", "grp", None, None),
        P("enc", "grp", None, None),
        P("enc", "grp"),
        P("enc", "grp"),
        P(),
        P(),
        P(),
        P(),
    )
    return jax.shard_map(
        shards, mesh=mesh, in_specs=placed, out_specs=P("enc", "grp", None), check_vma=False
    )
```

```python
import jax
import jax.numpy as jnp
from jax import lax
from jax.experimental import pallas as pl
from jax.experimental.pallas import tpu as pltpu
from jax.sharding import PartitionSpec as P

MESH = pl.DeviceIdType.MESH
F32 = jnp.float32
BF16 = jnp.bfloat16
LANES = 128
WIDTH = 1152
OUT_WIDTH = 4096
CLIPS = 64
PATCHES = 8
TOKENS = 3
RANKS = 64
ROWS = CLIPS * TOKENS
TILES = WIDTH // LANES
UNITS = ((6,), (0, 3), (1, 4), (2, 5), (7,), (8,))
PLACE = {tile: i for i, tile in enumerate(t for unit in UNITS for t in unit)}
FIRST = [sum(len(UNITS[v]) + 1 for v in range(u)) for u in range(len(UNITS))]
SLOT_TILES = sum(len(unit) + 1 for unit in UNITS)
LEADING = 7
LEAD = LEADING * LANES


def iota(shape, dim):
    return lax.broadcasted_iota(jnp.int32, shape, dim)


def for_peers(me, act, loop):
    x, y, core = me // 16, (me // 2) % 8, me % 2
    near = [
        ((x + dx) % 4) * 16 + (core + dcore) % 2 for dx in (2, 1, 3, 0) for dcore in (0, 1)
    ]

    def row(i, carry):
        dy = 4 + (1 - 2 * (i % 2)) * ((i + 1) // 2)
        at = ((y + dy) % 8) * 2
        for base in near:
            act(base + at)
        return carry

    if loop:
        lax.fori_loop(0, 7, row, 0)
    else:
        for i in range(7):
            row(i, 0)
    for i in (0, 1, 2, 3, 4, 5, 7):
        act(near[i] + 2 * y)


def unit_tiles(unit):
    return FIRST[unit], len(UNITS[unit]) + 1


def exchange(
    feats_hbm, win_hbm, counts_hbm, owners_hbm, gain_hbm, bias_hbm, weight_hbm,
    packed_ref, live_ref, total_ref, weight_ref,
    feats, win_ref, counts_ref, owners_ref, gain_ref, bias_ref,
    stats, mine, theirs, outgoing, arrived, leading,
    fetch_sem, z_send, z_recv, x_send, x_recv, own_sem,
):
    me = lax.axis_index("grp")
    frame = lax.axis_index("enc")
    last = lax.axis_size("enc") - 1
    pairs = (
        (feats_hbm, feats), (win_hbm, win_ref), (counts_hbm, counts_ref),
        (owners_hbm, owners_ref), (gain_hbm, gain_ref), (bias_hbm, bias_ref),
        (weight_hbm, weight_ref),
    )
    fetches = [
        pltpu.make_async_copy(source, target, fetch_sem.at[i])
        for i, (source, target) in enumerate(pairs)
    ]
    for fetch in fetches[:-1]:
        fetch.start()

    barrier = pltpu.get_barrier_semaphore()
    before = jnp.maximum(frame - 1, 0)
    after = jnp.minimum(frame + 1, last)

    def greet(peer):
        pl.semaphore_signal(barrier, inc=1, device_id={"grp": peer}, device_id_type=MESH)

    for_peers(me, greet, False)

    @pl.when(frame > 0)
    def _():
        pl.semaphore_signal(barrier, inc=1, device_id={"enc": before}, device_id_type=MESH)

    @pl.when(frame < last)
    def _():
        pl.semaphore_signal(barrier, inc=1, device_id={"enc": after}, device_id_type=MESH)

    for fetch in fetches[:-1]:
        fetch.wait()
    fetches[-1].start()
    group = 32

    def statistics(i, carry):
        at = pl.ds(pl.multiple_of(i * group, group), group)
        values = feats[at, :].astype(F32)
        mean = jnp.sum(values, axis=1, keepdims=True) * (1.0 / WIDTH)
        centred = values - mean
        var = jnp.sum(centred * centred, axis=1, keepdims=True) * (1.0 / WIDTH)
        stats[0, at, :] = jnp.broadcast_to(mean, (group, LANES))
        stats[1, at, :] = jnp.broadcast_to(lax.rsqrt(var + 1e-6), (group, LANES))
        return carry

    lax.fori_loop(0, CLIPS * PATCHES // group, statistics, 0)
    diagonal = iota((LANES, LANES), 0) == iota((LANES, LANES), 1)

    def as_row(which, start):
        column = stats[which, pl.ds(start, LANES), :]
        return jnp.sum(jnp.where(diagonal, column, 0.0), axis=0, keepdims=True)

    half = CLIPS // 2
    depth = half * PATCHES
    clip_diagonal = iota((CLIPS, CLIPS), 0) == iota((CLIPS, CLIPS), 1)

    def pick_column(token, w):
        row = win_ref[token, w : w + 1, :]
        return jnp.sum(jnp.where(clip_diagonal, row, 0), axis=1, keepdims=True)

    picked = [
        [pick_column(token, w) + PATCHES * (iota((CLIPS, 1), 0) % half) for w in range(4)]
        for token in range(TOKENS)
    ]
    for block in range(2):
        start = block * depth
        mean_row = jnp.concatenate([as_row(0, start), as_row(0, start + LANES)], axis=1)
        rstd_row = jnp.concatenate([as_row(1, start), as_row(1, start + LANES)], axis=1)
        parts = []
        for token in range(TOKENS):
            lanes = iota((half, depth), 1)
            weight = jnp.zeros((half, depth), F32)
            for w in range(4):
                picks = picked[token][w][block * half : (block + 1) * half]
                weight += jnp.where(picks == lanes, 0.25, 0.0)
            parts.append(weight)
        scaled = jnp.concatenate(parts, axis=0) * rstd_row
        shift = jnp.sum(scaled * mean_row, axis=1, keepdims=True)
        high = scaled.astype(BF16)
        rest = scaled - high.astype(F32)
        middle = rest.astype(BF16)
        low = (rest - middle.astype(F32)).astype(BF16)
        selector = jnp.concatenate([high, middle, low], axis=0)
        height = TOKENS * half
        for column in range(0, WIDTH, 2 * LANES):
            wide = min(2 * LANES, WIDTH - column)
            product = jnp.dot(
                selector, feats[pl.ds(start, depth), pl.ds(column, wide)],
                preferred_element_type=F32,
            )
            total = product[:height] + product[height : 2 * height] + product[2 * height :]
            total = total - shift
            for i in range(wide // LANES):
                tile = column // LANES + i
                pooled = total[:, i * LANES : (i + 1) * LANES] * gain_ref[tile : tile + 1, :]
                pooled = (pooled + bias_ref[tile : tile + 1, :]).astype(BF16)
                for token in range(TOKENS):
                    at = pl.ds(token * CLIPS + block * half, half)
                    mine[PLACE[tile], at, :] = pooled[token * half : (token + 1) * half]

    @pl.when(frame == last)
    def _():
        theirs[...] = mine[...]

    owner_row = owners_ref[...]
    count_row = counts_ref[...].astype(F32)
    rank = iota((2 * RANKS, CLIPS), 0) // 2
    odd = iota((2 * RANKS, CLIPS), 0) % 2
    owned = jnp.where(owner_row == rank, 1.0, 0.0)
    even_rows = jnp.where(odd == 0, owned, 0.0)
    odd_rows = jnp.where(odd == 1, owned, 0.0)
    place_matrix = jnp.concatenate([even_rows, odd_rows], axis=1).astype(BF16)
    third_matrix = even_rows.astype(BF16)
    count_column = jnp.sum(odd_rows * count_row, axis=1, keepdims=True)

    neighbours = jnp.minimum(frame, 1) + jnp.minimum(last - frame, 1)
    pl.semaphore_wait(barrier, RANKS - 1 + neighbours)

    def shift_copy(unit):
        at = pl.ds(PLACE[UNITS[unit][0]], len(UNITS[unit]))
        return pltpu.make_async_remote_copy(
            mine.at[at], theirs.at[at], z_send.at[unit], z_recv.at[unit],
            device_id={"enc": before}, device_id_type=MESH,
        )

    @pl.when(frame > 0)
    def _():
        for unit in range(len(UNITS)):
            shift_copy(unit).start()

    def own_copy(unit):
        at = pl.ds(*unit_tiles(unit))
        return pltpu.make_async_copy(
            outgoing.at[at, me], arrived.at[at, me], own_sem.at[unit]
        )

    for unit in range(len(UNITS)):
        @pl.when(frame < last)
        def _():
            shift_copy(unit).wait_recv()

        merged = []
        for tile in UNITS[unit]:
            place = PLACE[tile]
            merged.append(
                ((mine[place].astype(F32) + theirs[place].astype(F32)) * 0.5).astype(BF16)
            )
        first, tiles = unit_tiles(unit)
        for i, block in enumerate(merged):
            spread = jnp.dot(place_matrix, block[: 2 * CLIPS], preferred_element_type=F32)
            outgoing[first + i] = spread.astype(BF16).reshape(RANKS, 2, LANES)
        if tiles == 3:
            third = jnp.concatenate([block[2 * CLIPS :] for block in merged], axis=0)
            spread = jnp.dot(place_matrix, third, preferred_element_type=F32)
        else:
            spread = jnp.dot(third_matrix, merged[0][2 * CLIPS :], preferred_element_type=F32)
            if unit == 0:
                spread = spread + count_column
        outgoing[first + tiles - 1] = spread.astype(BF16).reshape(RANKS, 2, LANES)
        own_copy(unit).start()

        def send(peer):
            at = pl.ds(first, tiles)
            pltpu.make_async_remote_copy(
                outgoing.at[at, peer], arrived.at[at, me], x_send.at[unit], x_recv.at[unit],
                device_id={"grp": peer}, device_id_type=MESH,
            ).start()

        for_peers(me, send, True)

    def arrival(unit, sem):
        at = pl.ds(*unit_tiles(unit))
        everyone = pl.ds(0, RANKS - 1)
        return pltpu.make_async_copy(
            outgoing.at[at, everyone], arrived.at[at, everyone], sem.at[unit]
        )

    for unit in range(len(UNITS)):
        own_copy(unit).wait()
        arrival(unit, x_recv).wait()
        first, tiles = unit_tiles(unit)
        block = [arrived[first + i].reshape(2 * RANKS, LANES) for i in range(tiles)]
        if unit == 0:
            across = iota((2 * RANKS, 2 * RANKS), 1) // 2
            down = iota((2 * RANKS, 2 * RANKS), 0) // 2
            marked = iota((2 * RANKS, 2 * RANKS), 0) % 2 == 1
            earlier = jnp.where(marked & (down < across), 1.0, 0.0)
            same = jnp.where(marked & (down == across), 1.0, 0.0)
            table = jnp.concatenate([earlier, same], axis=1).astype(BF16)
            found = lax.dot_general(
                block[1], table, (((0,), (0,)), ((), ())), preferred_element_type=F32
            )
            opening = found[:1, : 2 * RANKS].astype(jnp.int32)
            count = found[:1, 2 * RANKS :].astype(jnp.int32)
            row = iota((ROWS, 2 * RANKS), 0)
            token = iota((ROWS, 2 * RANKS), 1) % 2
            pair = (row == opening + token) & (token < count)
            third = (row == opening + 2) & (count == 3)
            pair = jnp.where(pair, 1.0, 0.0)
            third_even = jnp.where(third & (token == 0), 1.0, 0.0)
            third_odd = jnp.where(third & (token == 1), 1.0, 0.0)
            live = jnp.sum(pair + third_even, axis=1, keepdims=True)
            live_ref[...] = jnp.broadcast_to(live, (ROWS, LANES))
            pack = (
                jnp.concatenate([pair, third_even], axis=1).astype(BF16),
                jnp.concatenate([pair, third_odd], axis=1).astype(BF16),
            )
        for i, tile in enumerate(UNITS[unit]):
            both = jnp.concatenate([block[i], block[tiles - 1]], axis=0)
            packed = jnp.dot(pack[i], both, preferred_element_type=F32).astype(BF16)
            if tile < LEADING:
                leading[:, tile * LANES : (tile + 1) * LANES] = packed
            else:
                at = (tile - LEADING) * LANES
                packed_ref[:, at : at + LANES] = packed
        if unit == 3:
            fetches[-1].wait()
            step = 512
            for column in range(0, OUT_WIDTH, step):
                at = pl.ds(column, step)
                total_ref[:, at] = jnp.dot(
                    leading[...], weight_ref[pl.ds(0, LEAD), at], preferred_element_type=F32
                )

    for unit in range(len(UNITS)):
        arrival(unit, x_send).wait()

    @pl.when(frame > 0)
    def _():
        for unit in range(len(UNITS)):
            shift_copy(unit).wait_send()


def project(packed_ref, live_ref, total_ref, weight_ref, bias_ref, result_ref, staged, sems):
    columns = staged.shape[2]
    shown = live_ref[:, :1] > 0.5

    def copy(n):
        at = pl.ds(n * columns, columns)
        return pltpu.make_async_copy(staged.at[n], result_ref.at[:, at], sems.at[n])

    for n in range(OUT_WIDTH // columns):
        at = pl.ds(n * columns, columns)
        product = total_ref[:, at] + jnp.dot(
            packed_ref[...], weight_ref[pl.ds(LEAD, WIDTH - LEAD), at],
            preferred_element_type=F32,
        )
        staged[n] = jnp.where(shown, product + bias_ref[:, at], 0.0).astype(BF16)
        copy(n).start()
    for n in range(OUT_WIDTH // columns):
        copy(n).wait()


def shards(patch_feats, windows, counts, owners, norm_gain, norm_bias, proj_weight, proj_bias):
    vmem = pl.BlockSpec(memory_space=pltpu.VMEM)
    hbm = pl.BlockSpec(memory_space=pltpu.HBM)
    units = len(UNITS)
    inputs = [
        pltpu.with_memory_space_constraint(array, pltpu.HBM)
        for array in (
            patch_feats.reshape(CLIPS * PATCHES, WIDTH), windows[0].transpose(1, 2, 0),
            counts, owners, norm_gain.reshape(TILES, LANES), norm_bias.reshape(TILES, LANES),
            proj_weight,
        )
    ]
    packed, live, total, weight = pl.pallas_call(
        exchange,
        name="exchange",
        out_shape=(
            jax.ShapeDtypeStruct((ROWS, WIDTH - LEAD), BF16),
            jax.ShapeDtypeStruct((ROWS, LANES), F32),
            jax.ShapeDtypeStruct((ROWS, OUT_WIDTH), F32),
            jax.ShapeDtypeStruct((WIDTH, OUT_WIDTH), BF16),
        ),
        in_specs=[hbm] * len(inputs),
        out_specs=(vmem,) * 4,
        scratch_shapes=[pltpu.VMEM(array.shape, array.dtype) for array in inputs[:-1]] + [
            pltpu.VMEM((2, CLIPS * PATCHES, LANES), F32),
            pltpu.VMEM((TILES, ROWS, LANES), BF16),
            pltpu.VMEM((TILES, ROWS, LANES), BF16),
            pltpu.VMEM((SLOT_TILES, RANKS, 2, LANES), BF16),
            pltpu.VMEM((SLOT_TILES, RANKS, 2, LANES), BF16),
            pltpu.VMEM((ROWS, LEAD), BF16),
            pltpu.SemaphoreType.DMA((len(inputs),)),
        ] + [pltpu.SemaphoreType.DMA((units,))] * 5,
        compiler_params=pltpu.CompilerParams(
            collective_id=0, has_side_effects=True, vmem_limit_bytes=24 << 20
        ),
        cost_estimate=pl.CostEstimate(
            flops=60_000_000_000, bytes_accessed=4_000_000, transcendentals=0
        ),
    )(*inputs)
    step = 512
    result = pl.pallas_call(
        project,
        name="project",
        out_shape=jax.ShapeDtypeStruct((ROWS, OUT_WIDTH), BF16),
        in_specs=[vmem] * 5,
        out_specs=hbm,
        scratch_shapes=[
            pltpu.VMEM((OUT_WIDTH // step, ROWS, step), BF16),
            pltpu.SemaphoreType.DMA((OUT_WIDTH // step,)),
        ],
        compiler_params=pltpu.CompilerParams(vmem_limit_bytes=16 << 20),
        cost_estimate=pl.CostEstimate(
            flops=2 * ROWS * WIDTH * OUT_WIDTH, bytes_accessed=12_000_000, transcendentals=0
        ),
    )(packed, live, total, weight, proj_bias.reshape(1, OUT_WIDTH))
    return result[None]


def solution(mesh):
    placed = (
        P("enc", "grp", None, None),
        P("enc", "grp", None, None),
        P("enc", "grp"),
        P("enc", "grp"),
        P(),
        P(),
        P(),
        P(),
    )
    return jax.shard_map(
        shards, mesh=mesh, in_specs=placed, out_specs=P("enc", "grp", None), check_vma=False
    )
```

```python
import jax
import jax.numpy as jnp
from jax import lax
from jax.experimental import pallas as pl
from jax.experimental.pallas import tpu as pltpu
from jax.sharding import PartitionSpec as P

MESH = pl.DeviceIdType.MESH
F32 = jnp.float32
BF16 = jnp.bfloat16
LANES = 128
WIDTH = 1152
OUT_WIDTH = 4096
CLIPS = 64
PATCHES = 8
TOKENS = 3
RANKS = 64
ROWS = CLIPS * TOKENS
TILES = WIDTH // LANES
GROUPS = (
    ((6,), (6,), 0, 2),
    ((0, 3), (0, 3), 2, 3),
    ((1, 4), (1, 4), 5, 3),
    ((2, 5), (2, 5), 8, 3),
    ((7,), (), 11, 1),
    ((8,), (7, 8), 12, 2),
)
PLACE = {tile: i for i, tile in enumerate(t for group in GROUPS for t in group[0])}
PAIR_AT = {tile: g[2] + i for g in GROUPS for i, tile in enumerate(g[0])}
SLOT_TILES = 14
PIECE = 32
LEADING = 7
LEAD = LEADING * LANES


def iota(shape, dim):
    return lax.broadcasted_iota(jnp.int32, shape, dim)


def for_peers(me, act, loop):
    x, y, core = me // 16, (me // 2) % 8, me % 2
    near = [
        ((x + dx) % 4) * 16 + (core + dcore) % 2 for dx in (2, 1, 3, 0) for dcore in (0, 1)
    ]

    def row(i, carry):
        dy = 4 + (1 - 2 * (i % 2)) * ((i + 1) // 2)
        at = ((y + dy) % 8) * 2
        for base in near:
            act(base + at)
        return carry

    if loop:
        lax.fori_loop(0, 7, row, 0)
    else:
        for i in range(7):
            row(i, 0)
    for i in (0, 1, 2, 3, 4, 5, 7):
        act(near[i] + 2 * y)


def exchange(
    feats_hbm, win_hbm, counts_hbm, owners_hbm, gain_hbm, bias_hbm, weight_hbm,
    packed_ref, live_ref, total_ref, weight_ref,
    feats, win_ref, counts_ref, owners_ref, gain_ref, bias_ref,
    stats, mine, theirs, outgoing, arrived, leading,
    fetch_sem, z_send, z_recv, x_send, x_recv, own_sem,
):
    me = lax.axis_index("grp")
    frame = lax.axis_index("enc")
    last = lax.axis_size("enc") - 1
    pairs = (
        (feats_hbm, feats), (win_hbm, win_ref), (counts_hbm, counts_ref),
        (owners_hbm, owners_ref), (gain_hbm, gain_ref), (bias_hbm, bias_ref),
        (weight_hbm, weight_ref),
    )
    fetches = [
        pltpu.make_async_copy(source, target, fetch_sem.at[i])
        for i, (source, target) in enumerate(pairs)
    ]
    for fetch in fetches[:-1]:
        fetch.start()

    barrier = pltpu.get_barrier_semaphore()
    before = jnp.maximum(frame - 1, 0)
    after = jnp.minimum(frame + 1, last)

    def greet(peer):
        pl.semaphore_signal(barrier, inc=1, device_id={"grp": peer}, device_id_type=MESH)

    for_peers(me, greet, False)

    @pl.when(frame > 0)
    def _():
        pl.semaphore_signal(barrier, inc=1, device_id={"enc": before}, device_id_type=MESH)

    @pl.when(frame < last)
    def _():
        pl.semaphore_signal(barrier, inc=1, device_id={"enc": after}, device_id_type=MESH)

    for fetch in fetches[:-1]:
        fetch.wait()
    fetches[-1].start()
    group = 32

    def statistics(i, carry):
        at = pl.ds(pl.multiple_of(i * group, group), group)
        values = feats[at, :].astype(F32)
        mean = jnp.sum(values, axis=1, keepdims=True) * (1.0 / WIDTH)
        centred = values - mean
        var = jnp.sum(centred * centred, axis=1, keepdims=True) * (1.0 / WIDTH)
        stats[0, at, :] = jnp.broadcast_to(mean, (group, LANES))
        stats[1, at, :] = jnp.broadcast_to(lax.rsqrt(var + 1e-6), (group, LANES))
        return carry

    lax.fori_loop(0, CLIPS * PATCHES // group, statistics, 0)
    diagonal = iota((LANES, LANES), 0) == iota((LANES, LANES), 1)

    def as_row(which, start):
        column = stats[which, pl.ds(start, LANES), :]
        return jnp.sum(jnp.where(diagonal, column, 0.0), axis=0, keepdims=True)

    half = CLIPS // 2
    depth = half * PATCHES
    clip_diagonal = iota((CLIPS, CLIPS), 0) == iota((CLIPS, CLIPS), 1)

    def pick_column(token, w):
        row = win_ref[token, w : w + 1, :]
        return jnp.sum(jnp.where(clip_diagonal, row, 0), axis=1, keepdims=True)

    picked = [
        [pick_column(token, w) + PATCHES * (iota((CLIPS, 1), 0) % half) for w in range(4)]
        for token in range(TOKENS)
    ]
    for block in range(2):
        start = block * depth
        mean_row = jnp.concatenate([as_row(0, start), as_row(0, start + LANES)], axis=1)
        rstd_row = jnp.concatenate([as_row(1, start), as_row(1, start + LANES)], axis=1)
        parts = []
        for token in range(TOKENS):
            lanes = iota((half, depth), 1)
            weight = jnp.zeros((half, depth), F32)
            for w in range(4):
                picks = picked[token][w][block * half : (block + 1) * half]
                weight += jnp.where(picks == lanes, 0.25, 0.0)
            parts.append(weight)
        scaled = jnp.concatenate(parts, axis=0) * rstd_row
        shift = jnp.sum(scaled * mean_row, axis=1, keepdims=True)
        high = scaled.astype(BF16)
        rest = scaled - high.astype(F32)
        middle = rest.astype(BF16)
        low = (rest - middle.astype(F32)).astype(BF16)
        selector = jnp.concatenate([high, middle, low], axis=0)
        height = TOKENS * half
        for column in range(0, WIDTH, 2 * LANES):
            wide = min(2 * LANES, WIDTH - column)
            product = jnp.dot(
                selector, feats[pl.ds(start, depth), pl.ds(column, wide)],
                preferred_element_type=F32,
            )
            total = product[:height] + product[height : 2 * height] + product[2 * height :]
            total = total - shift
            for i in range(wide // LANES):
                tile = column // LANES + i
                pooled = total[:, i * LANES : (i + 1) * LANES] * gain_ref[tile : tile + 1, :]
                pooled = (pooled + bias_ref[tile : tile + 1, :]).astype(BF16)
                for token in range(TOKENS):
                    at = pl.ds(token * CLIPS + block * half, half)
                    mine[PLACE[tile], at, :] = pooled[token * half : (token + 1) * half]

    @pl.when(frame == last)
    def _():
        theirs[...] = mine[...]

    owner_row = owners_ref[...]
    count_row = counts_ref[...].astype(F32)
    rank = iota((2 * RANKS, CLIPS), 0) // 2
    odd = iota((2 * RANKS, CLIPS), 0) % 2
    owned = jnp.where(owner_row == rank, 1.0, 0.0)
    even_rows = jnp.where(odd == 0, owned, 0.0)
    odd_rows = jnp.where(odd == 1, owned, 0.0)
    place_matrix = jnp.concatenate([even_rows, odd_rows], axis=1).astype(BF16)
    third_matrix = even_rows.astype(BF16)
    count_column = jnp.sum(odd_rows * count_row, axis=1, keepdims=True)

    neighbours = jnp.minimum(frame, 1) + jnp.minimum(last - frame, 1)
    pl.semaphore_wait(barrier, RANKS - 1 + neighbours)

    pieces = ROWS // PIECE

    @pl.when(frame > 0)
    def _():
        def shift(i, carry):
            place = i // pieces
            at = pl.ds(pl.multiple_of((i % pieces) * PIECE, PIECE), PIECE)
            pltpu.make_async_remote_copy(
                mine.at[place, at], theirs.at[place, at], z_send.at[place], z_recv.at[place],
                device_id={"enc": before}, device_id_type=MESH,
            ).start()
            return carry

        lax.fori_loop(0, TILES * pieces, shift, 0)

    def own_copy(i):
        at = pl.ds(*GROUPS[i][2:])
        return pltpu.make_async_copy(outgoing.at[at, me], arrived.at[at, me], own_sem.at[i])

    merged = {}
    for i, (tiles, thirds, first, depth) in enumerate(GROUPS):
        for tile in tiles:
            place = PLACE[tile]

            @pl.when(frame < last)
            def _():
                pltpu.make_async_copy(mine.at[place], theirs.at[place], z_recv.at[place]).wait()

            merged[tile] = (
                (mine[place].astype(F32) + theirs[place].astype(F32)) * 0.5
            ).astype(BF16)
            spread = jnp.dot(
                place_matrix, merged[tile][: 2 * CLIPS], preferred_element_type=F32
            )
            outgoing[PAIR_AT[tile]] = spread.astype(BF16).reshape(RANKS, 2, LANES)
        if thirds:
            rows = [merged[tile][2 * CLIPS :] for tile in thirds]
            if len(rows) == 2:
                rows = jnp.concatenate(rows, axis=0)
                spread = jnp.dot(place_matrix, rows, preferred_element_type=F32)
            else:
                spread = jnp.dot(third_matrix, rows[0], preferred_element_type=F32)
                spread = spread + count_column
            outgoing[first + depth - 1] = spread.astype(BF16).reshape(RANKS, 2, LANES)
        own_copy(i).start()

        def send(peer):
            at = pl.ds(first, depth)
            pltpu.make_async_remote_copy(
                outgoing.at[at, peer], arrived.at[at, me], x_send.at[i], x_recv.at[i],
                device_id={"grp": peer}, device_id_type=MESH,
            ).start()

        for_peers(me, send, True)

    def arrival(i, sem):
        at = pl.ds(*GROUPS[i][2:])
        everyone = pl.ds(0, RANKS - 1)
        return pltpu.make_async_copy(
            outgoing.at[at, everyone], arrived.at[at, everyone], sem.at[i]
        )

    def slot_tile(i):
        return arrived[i].reshape(2 * RANKS, LANES)

    for i, (tiles, thirds, first, depth) in enumerate(GROUPS):
        own_copy(i).wait()
        arrival(i, x_recv).wait()
        if i == 0:
            across = iota((2 * RANKS, 2 * RANKS), 1) // 2
            down = iota((2 * RANKS, 2 * RANKS), 0) // 2
            marked = iota((2 * RANKS, 2 * RANKS), 0) % 2 == 1
            earlier = jnp.where(marked & (down < across), 1.0, 0.0)
            same = jnp.where(marked & (down == across), 1.0, 0.0)
            table = jnp.concatenate([earlier, same], axis=1).astype(BF16)
            found = lax.dot_general(
                slot_tile(1), table, (((0,), (0,)), ((), ())), preferred_element_type=F32
            )
            opening = found[:1, : 2 * RANKS].astype(jnp.int32)
            count = found[:1, 2 * RANKS :].astype(jnp.int32)
            row = iota((ROWS, 2 * RANKS), 0)
            token = iota((ROWS, 2 * RANKS), 1) % 2
            pair = (row == opening + token) & (token < count)
            third = (row == opening + 2) & (count == 3)
            pair = jnp.where(pair, 1.0, 0.0)
            third_even = jnp.where(third & (token == 0), 1.0, 0.0)
            third_odd = jnp.where(third & (token == 1), 1.0, 0.0)
            live = jnp.sum(pair + third_even, axis=1, keepdims=True)
            live_ref[...] = jnp.broadcast_to(live, (ROWS, LANES))
            pack = (
                jnp.concatenate([pair, third_even], axis=1).astype(BF16),
                jnp.concatenate([pair, third_odd], axis=1).astype(BF16),
            )
        if thirds:
            shared = slot_tile(first + depth - 1)
        for side, tile in enumerate(thirds):
            both = jnp.concatenate([slot_tile(PAIR_AT[tile]), shared], axis=0)
            packed = jnp.dot(pack[side], both, preferred_element_type=F32).astype(BF16)
            if tile < LEADING:
                leading[:, tile * LANES : (tile + 1) * LANES] = packed
            else:
                at = (tile - LEADING) * LANES
                packed_ref[:, at : at + LANES] = packed
        if i == 3:
            fetches[-1].wait()
            step = 512
            for column in range(0, OUT_WIDTH, step):
                at = pl.ds(column, step)
                total_ref[:, at] = jnp.dot(
                    leading[...], weight_ref[pl.ds(0, LEAD), at], preferred_element_type=F32
                )

    for i in range(len(GROUPS)):
        arrival(i, x_send).wait()

    @pl.when(frame > 0)
    def _():
        for place in range(TILES):
            pltpu.make_async_copy(mine.at[place], theirs.at[place], z_send.at[place]).wait()


def project(packed_ref, live_ref, total_ref, weight_ref, bias_ref, result_ref, staged, sems):
    columns = staged.shape[2]
    shown = live_ref[:, :1] > 0.5

    def copy(n):
        at = pl.ds(n * columns, columns)
        return pltpu.make_async_copy(staged.at[n], result_ref.at[:, at], sems.at[n])

    for n in range(OUT_WIDTH // columns):
        at = pl.ds(n * columns, columns)
        product = total_ref[:, at] + jnp.dot(
            packed_ref[...], weight_ref[pl.ds(LEAD, WIDTH - LEAD), at],
            preferred_element_type=F32,
        )
        staged[n] = jnp.where(shown, product + bias_ref[:, at], 0.0).astype(BF16)
        copy(n).start()
    for n in range(OUT_WIDTH // columns):
        copy(n).wait()


def shards(patch_feats, windows, counts, owners, norm_gain, norm_bias, proj_weight, proj_bias):
    vmem = pl.BlockSpec(memory_space=pltpu.VMEM)
    hbm = pl.BlockSpec(memory_space=pltpu.HBM)
    groups = len(GROUPS)
    inputs = [
        pltpu.with_memory_space_constraint(array, pltpu.HBM)
        for array in (
            patch_feats.reshape(CLIPS * PATCHES, WIDTH), windows[0].transpose(1, 2, 0),
            counts, owners, norm_gain.reshape(TILES, LANES), norm_bias.reshape(TILES, LANES),
            proj_weight,
        )
    ]
    packed, live, total, weight = pl.pallas_call(
        exchange,
        name="exchange",
        out_shape=(
            jax.ShapeDtypeStruct((ROWS, WIDTH - LEAD), BF16),
            jax.ShapeDtypeStruct((ROWS, LANES), F32),
            jax.ShapeDtypeStruct((ROWS, OUT_WIDTH), F32),
            jax.ShapeDtypeStruct((WIDTH, OUT_WIDTH), BF16),
        ),
        in_specs=[hbm] * len(inputs),
        out_specs=(vmem,) * 4,
        scratch_shapes=[pltpu.VMEM(array.shape, array.dtype) for array in inputs[:-1]] + [
            pltpu.VMEM((2, CLIPS * PATCHES, LANES), F32),
            pltpu.VMEM((TILES, ROWS, LANES), BF16),
            pltpu.VMEM((TILES, ROWS, LANES), BF16),
            pltpu.VMEM((SLOT_TILES, RANKS, 2, LANES), BF16),
            pltpu.VMEM((SLOT_TILES, RANKS, 2, LANES), BF16),
            pltpu.VMEM((ROWS, LEAD), BF16),
            pltpu.SemaphoreType.DMA((len(inputs),)),
        ] + [pltpu.SemaphoreType.DMA((TILES,))] * 2 + [pltpu.SemaphoreType.DMA((groups,))] * 3,
        compiler_params=pltpu.CompilerParams(
            collective_id=0, has_side_effects=True, vmem_limit_bytes=24 << 20
        ),
        cost_estimate=pl.CostEstimate(
            flops=60_000_000_000, bytes_accessed=4_000_000, transcendentals=0
        ),
    )(*inputs)
    step = 512
    result = pl.pallas_call(
        project,
        name="project",
        out_shape=jax.ShapeDtypeStruct((ROWS, OUT_WIDTH), BF16),
        in_specs=[vmem] * 5,
        out_specs=hbm,
        scratch_shapes=[
            pltpu.VMEM((OUT_WIDTH // step, ROWS, step), BF16),
            pltpu.SemaphoreType.DMA((OUT_WIDTH // step,)),
        ],
        compiler_params=pltpu.CompilerParams(vmem_limit_bytes=16 << 20),
        cost_estimate=pl.CostEstimate(
            flops=2 * ROWS * WIDTH * OUT_WIDTH, bytes_accessed=12_000_000, transcendentals=0
        ),
    )(packed, live, total, weight, proj_bias.reshape(1, OUT_WIDTH))
    return result[None]


def solution(mesh):
    placed = (
        P("enc", "grp", None, None),
        P("enc", "grp", None, None),
        P("enc", "grp"),
        P("enc", "grp"),
        P(),
        P(),
        P(),
        P(),
    )
    return jax.shard_map(
        shards, mesh=mesh, in_specs=placed, out_specs=P("enc", "grp", None), check_vma=False
    )
```

```python
import jax
import jax.numpy as jnp
from jax import lax
from jax.experimental import pallas as pl
from jax.experimental.pallas import tpu as pltpu
from jax.sharding import PartitionSpec as P

MESH = pl.DeviceIdType.MESH
F32 = jnp.float32
BF16 = jnp.bfloat16
LANES = 128
WIDTH = 1152
OUT_WIDTH = 4096
CLIPS = 64
PATCHES = 8
TOKENS = 3
RANKS = 64
ROWS = CLIPS * TOKENS
TILES = WIDTH // LANES
GROUPS = (
    ((6,), (), 0, 1),
    ((0, 3), (6, 0, 3), 1, 4),
    ((1, 4), (1, 4), 5, 3),
    ((2, 5), (2, 5), 8, 3),
    ((7,), (), 11, 1),
    ((8,), (7, 8), 12, 2),
)
PLACE = {tile: i for i, tile in enumerate(t for group in GROUPS for t in group[0])}
PAIR_AT = {tile: g[2] + i for g in GROUPS for i, tile in enumerate(g[0])}
THIRD_AT = {6: 3, 0: 4, 3: 4, 1: 7, 4: 7, 2: 10, 5: 10, 7: 13, 8: 13}
SLOT_TILES = 14
PIECE = 32
LEADING = 7
LEAD = LEADING * LANES


def iota(shape, dim):
    return lax.broadcasted_iota(jnp.int32, shape, dim)


def for_peers(me, act):
    x, y, core = me // 16, (me // 2) % 8, me % 2
    near = [
        ((x + dx) % 4) * 16 + (core + dcore) % 2 for dx in (2, 1, 3, 0) for dcore in (0, 1)
    ]

    def row(i, carry):
        dy = 4 + (1 - 2 * (i % 2)) * ((i + 1) // 2)
        at = ((y + dy) % 8) * 2
        for base in near:
            act(base + at)
        return carry

    lax.fori_loop(0, 7, row, 0)
    for i in (0, 1, 2, 3, 4, 5, 7):
        act(near[i] + 2 * y)


def exchange(
    feats_hbm, win_hbm, counts_hbm, owners_hbm, gain_hbm, bias_hbm, weight_hbm,
    packed_ref, live_ref, total_ref, weight_ref,
    feats, win_ref, counts_ref, owners_ref, gain_ref, bias_ref,
    stats, mine, theirs, outgoing, arrived, leading,
    fetch_sem, z_send, z_recv, x_send, x_recv, own_sem, column_sem, row_sem,
):
    me = lax.axis_index("grp")
    frame = lax.axis_index("enc")
    last = lax.axis_size("enc") - 1
    pairs = (
        (feats_hbm, feats), (win_hbm, win_ref), (counts_hbm, counts_ref),
        (owners_hbm, owners_ref), (gain_hbm, gain_ref), (bias_hbm, bias_ref),
        (weight_hbm, weight_ref),
    )
    fetches = [
        pltpu.make_async_copy(source, target, fetch_sem.at[i])
        for i, (source, target) in enumerate(pairs)
    ]
    for fetch in fetches[:-1]:
        fetch.start()

    barrier = pltpu.get_barrier_semaphore()
    before = jnp.maximum(frame - 1, 0)
    after = jnp.minimum(frame + 1, last)

    x, y, core = me // 16, (me // 2) % 8, me % 2
    column_peers = [16 * x + 2 * ((y + dy) % 8) + core for dy in (2, 6, 1, 7)]
    row_peers = [
        16 * ((x + dx) % 4) + 2 * y + (core + dcore) % 2
        for dx, dcore in ((2, 1), (2, 0), (1, 1), (3, 1), (1, 0), (3, 0), (0, 1))
    ]

    def tell(sem, peers):
        for peer in peers:
            pl.semaphore_signal(sem, inc=1, device_id={"grp": peer}, device_id_type=MESH)

    tell(barrier, column_peers + row_peers)

    @pl.when(frame > 0)
    def _():
        pl.semaphore_signal(barrier, inc=1, device_id={"enc": before}, device_id_type=MESH)

    @pl.when(frame < last)
    def _():
        pl.semaphore_signal(barrier, inc=1, device_id={"enc": after}, device_id_type=MESH)

    for fetch in fetches[:-1]:
        fetch.wait()
    fetches[-1].start()
    group = 32

    def statistics(i, carry):
        at = pl.ds(pl.multiple_of(i * group, group), group)
        values = feats[at, :].astype(F32)
        mean = jnp.sum(values, axis=1, keepdims=True) * (1.0 / WIDTH)
        centred = values - mean
        var = jnp.sum(centred * centred, axis=1, keepdims=True) * (1.0 / WIDTH)
        stats[0, at, :] = jnp.broadcast_to(mean, (group, LANES))
        stats[1, at, :] = jnp.broadcast_to(lax.rsqrt(var + 1e-6), (group, LANES))
        return carry

    lax.fori_loop(0, CLIPS * PATCHES // group, statistics, 0, unroll=2)
    diagonal = iota((LANES, LANES), 0) == iota((LANES, LANES), 1)

    def as_row(which, start):
        column = stats[which, pl.ds(start, LANES), :]
        return jnp.sum(jnp.where(diagonal, column, 0.0), axis=0, keepdims=True)

    half = CLIPS // 2
    depth = half * PATCHES
    clip_diagonal = iota((CLIPS, CLIPS), 0) == iota((CLIPS, CLIPS), 1)

    def pick_column(token, w):
        row = win_ref[token, w : w + 1, :]
        return jnp.sum(jnp.where(clip_diagonal, row, 0), axis=1, keepdims=True)

    picked = [
        [pick_column(token, w) + PATCHES * (iota((CLIPS, 1), 0) % half) for w in range(4)]
        for token in range(TOKENS)
    ]
    for block in range(2):
        start = block * depth
        mean_row = jnp.concatenate([as_row(0, start), as_row(0, start + LANES)], axis=1)
        rstd_row = jnp.concatenate([as_row(1, start), as_row(1, start + LANES)], axis=1)
        parts = []
        for token in range(TOKENS):
            lanes = iota((half, depth), 1)
            weight = jnp.zeros((half, depth), F32)
            for w in range(4):
                picks = picked[token][w][block * half : (block + 1) * half]
                weight += jnp.where(picks == lanes, 0.25, 0.0)
            parts.append(weight)
        scaled = jnp.concatenate(parts, axis=0) * rstd_row
        shift = jnp.sum(scaled * mean_row, axis=1, keepdims=True)
        high = scaled.astype(BF16)
        rest = scaled - high.astype(F32)
        middle = rest.astype(BF16)
        low = (rest - middle.astype(F32)).astype(BF16)
        selector = jnp.concatenate([high, middle, low], axis=0)
        height = TOKENS * half
        for column in range(0, WIDTH, 2 * LANES):
            wide = min(2 * LANES, WIDTH - column)
            product = jnp.dot(
                selector, feats[pl.ds(start, depth), pl.ds(column, wide)],
                preferred_element_type=F32,
            )
            total = product[:height] + product[height : 2 * height] + product[2 * height :]
            total = total - shift
            for i in range(wide // LANES):
                tile = column // LANES + i
                pooled = total[:, i * LANES : (i + 1) * LANES] * gain_ref[tile : tile + 1, :]
                pooled = (pooled + bias_ref[tile : tile + 1, :]).astype(BF16)
                for token in range(TOKENS):
                    at = pl.ds(token * CLIPS + block * half, half)
                    mine[PLACE[tile], at, :] = pooled[token * half : (token + 1) * half]

    @pl.when(frame == last)
    def _():
        theirs[...] = mine[...]

    owner_row = owners_ref[...]
    count_row = counts_ref[...].astype(F32)
    rank = iota((2 * RANKS, CLIPS), 0) // 2
    odd = iota((2 * RANKS, CLIPS), 0) % 2
    owned = jnp.where(owner_row == rank, 1.0, 0.0)
    even_rows = jnp.where(odd == 0, owned, 0.0)
    odd_rows = jnp.where(odd == 1, owned, 0.0)
    place_matrix = jnp.concatenate([even_rows, odd_rows], axis=1).astype(BF16)
    third_matrix = even_rows.astype(BF16)
    count_column = jnp.sum(odd_rows * count_row, axis=1, keepdims=True)

    neighbours = jnp.minimum(frame, 1) + jnp.minimum(last - frame, 1)
    pl.semaphore_wait(barrier, len(column_peers) + len(row_peers) + neighbours)
    tell(column_sem, column_peers)

    pieces = ROWS // PIECE
    parts = [(0, 2 * CLIPS, 0), (0, CLIPS, TILES)] + [(p, ROWS, p) for p in range(1, TILES)]

    def shift(place, piece, sem):
        at = pl.ds(pl.multiple_of(piece * PIECE, PIECE), PIECE)
        pltpu.make_async_remote_copy(
            mine.at[place, at], theirs.at[place, at], z_send.at[sem], z_recv.at[sem],
            device_id={"enc": before}, device_id_type=MESH,
        ).start()

    @pl.when(frame > 0)
    def _():
        pairs_end = 2 * CLIPS // PIECE
        for piece in range(pieces):
            shift(0, piece, 0 if piece < pairs_end else TILES)

        def rest(i, carry):
            shift(i // pieces, i % pieces, i // pieces)
            return carry

        lax.fori_loop(pieces, TILES * pieces, rest, 0)

    pl.semaphore_wait(column_sem, len(column_peers))
    tell(row_sem, row_peers)
    pl.semaphore_wait(row_sem, len(row_peers))

    def shift_wait(part, sems):
        place, rows, sem = parts[part]
        at = pl.ds(0, rows)
        pltpu.make_async_copy(mine.at[place, at], theirs.at[place, at], sems.at[sem]).wait()

    def shifted(part):
        @pl.when(frame < last)
        def _():
            shift_wait(part, z_recv)

    def merge(place, at):
        return ((mine[place, at, :].astype(F32) + theirs[place, at, :].astype(F32)) * 0.5).astype(
            BF16
        )

    def lay_out(matrix, rows):
        return jnp.dot(matrix, rows, preferred_element_type=F32)

    def put(at, spread):
        outgoing[at] = spread.astype(BF16).reshape(RANKS, 2, LANES)

    def own_copy(i):
        at = pl.ds(*GROUPS[i][2:])
        return pltpu.make_async_copy(outgoing.at[at, me], arrived.at[at, me], own_sem.at[i])

    thirds_of = {}
    first_two, third_rows = pl.ds(0, 2 * CLIPS), pl.ds(2 * CLIPS, CLIPS)
    for i, (tiles, thirds, first, depth) in enumerate(GROUPS):
        for tile in tiles:
            place = PLACE[tile]
            shifted(place + 1 if place else 0)
            put(PAIR_AT[tile], lay_out(place_matrix, merge(place, first_two)))
            if place:
                thirds_of[tile] = merge(place, third_rows)
        if i == 1:
            shifted(1)
            put(THIRD_AT[6], lay_out(third_matrix, merge(0, third_rows)) + count_column)
        if thirds:
            rows = jnp.concatenate([thirds_of[tile] for tile in thirds[-2:]], axis=0)
            put(THIRD_AT[thirds[-1]], lay_out(place_matrix, rows))
        own_copy(i).start()

        def send(peer):
            at = pl.ds(first, depth)
            pltpu.make_async_remote_copy(
                outgoing.at[at, peer], arrived.at[at, me], x_send.at[i], x_recv.at[i],
                device_id={"grp": peer}, device_id_type=MESH,
            ).start()

        for_peers(me, send)

    def arrival(i, sem):
        at = pl.ds(*GROUPS[i][2:])
        everyone = pl.ds(0, RANKS - 1)
        return pltpu.make_async_copy(
            outgoing.at[at, everyone], arrived.at[at, everyone], sem.at[i]
        )

    def slot_tile(i):
        return arrived[i].reshape(2 * RANKS, LANES)

    for i, (tiles, thirds, first, depth) in enumerate(GROUPS):
        own_copy(i).wait()
        arrival(i, x_recv).wait()
        if i == 1:
            across = iota((2 * RANKS, 2 * RANKS), 1) // 2
            down = iota((2 * RANKS, 2 * RANKS), 0) // 2
            marked = iota((2 * RANKS, 2 * RANKS), 0) % 2 == 1
            earlier = jnp.where(marked & (down < across), 1.0, 0.0)
            same = jnp.where(marked & (down == across), 1.0, 0.0)
            table = jnp.concatenate([earlier, same], axis=1).astype(BF16)
            found = lax.dot_general(
                slot_tile(THIRD_AT[6]), table, (((0,), (0,)), ((), ())), preferred_element_type=F32
            )
            opening = found[:1, : 2 * RANKS].astype(jnp.int32)
            count = found[:1, 2 * RANKS :].astype(jnp.int32)
            row = iota((ROWS, 2 * RANKS), 0)
            token = iota((ROWS, 2 * RANKS), 1) % 2
            pair = (row == opening + token) & (token < count)
            third = (row == opening + 2) & (count == 3)
            pair = jnp.where(pair, 1.0, 0.0)
            third_even = jnp.where(third & (token == 0), 1.0, 0.0)
            third_odd = jnp.where(third & (token == 1), 1.0, 0.0)
            live = jnp.sum(pair + third_even, axis=1, keepdims=True)
            live_ref[...] = jnp.broadcast_to(live, (ROWS, LANES))
            pack = (
                jnp.concatenate([pair, third_even], axis=1).astype(BF16),
                jnp.concatenate([pair, third_odd], axis=1).astype(BF16),
            )
        for tile in thirds:
            side = tile in (3, 4, 5, 8)
            both = jnp.concatenate(
                [slot_tile(PAIR_AT[tile]), slot_tile(THIRD_AT[tile])], axis=0
            )
            packed = jnp.dot(pack[side], both, preferred_element_type=F32).astype(BF16)
            if tile < LEADING:
                leading[:, tile * LANES : (tile + 1) * LANES] = packed
            else:
                at = (tile - LEADING) * LANES
                packed_ref[:, at : at + LANES] = packed
        if i == 3:
            fetches[-1].wait()
            step = 512
            for column in range(0, OUT_WIDTH, step):
                at = pl.ds(column, step)
                total_ref[:, at] = jnp.dot(
                    leading[...], weight_ref[pl.ds(0, LEAD), at], preferred_element_type=F32
                )

    for i in range(len(GROUPS)):
        arrival(i, x_send).wait()

    @pl.when(frame > 0)
    def _():
        for part in range(len(parts)):
            shift_wait(part, z_send)


def project(packed_ref, live_ref, total_ref, weight_ref, bias_ref, result_ref, staged, sems):
    columns = staged.shape[2]
    shown = live_ref[:, :1] > 0.5

    def copy(n):
        at = pl.ds(n * columns, columns)
        return pltpu.make_async_copy(staged.at[n], result_ref.at[:, at], sems.at[n])

    for n in range(OUT_WIDTH // columns):
        at = pl.ds(n * columns, columns)
        product = total_ref[:, at] + jnp.dot(
            packed_ref[...], weight_ref[pl.ds(LEAD, WIDTH - LEAD), at],
            preferred_element_type=F32,
        )
        staged[n] = jnp.where(shown, product + bias_ref[:, at], 0.0).astype(BF16)
        copy(n).start()
    for n in range(OUT_WIDTH // columns):
        copy(n).wait()


def shards(patch_feats, windows, counts, owners, norm_gain, norm_bias, proj_weight, proj_bias):
    vmem = pl.BlockSpec(memory_space=pltpu.VMEM)
    hbm = pl.BlockSpec(memory_space=pltpu.HBM)
    groups = len(GROUPS)
    inputs = [
        pltpu.with_memory_space_constraint(array, pltpu.HBM)
        for array in (
            patch_feats.reshape(CLIPS * PATCHES, WIDTH), windows[0].transpose(1, 2, 0),
            counts, owners, norm_gain.reshape(TILES, LANES), norm_bias.reshape(TILES, LANES),
            proj_weight,
        )
    ]
    packed, live, total, weight = pl.pallas_call(
        exchange,
        name="exchange",
        out_shape=(
            jax.ShapeDtypeStruct((ROWS, WIDTH - LEAD), BF16),
            jax.ShapeDtypeStruct((ROWS, LANES), F32),
            jax.ShapeDtypeStruct((ROWS, OUT_WIDTH), F32),
            jax.ShapeDtypeStruct((WIDTH, OUT_WIDTH), BF16),
        ),
        in_specs=[hbm] * len(inputs),
        out_specs=(vmem,) * 4,
        scratch_shapes=[pltpu.VMEM(array.shape, array.dtype) for array in inputs[:-1]] + [
            pltpu.VMEM((2, CLIPS * PATCHES, LANES), F32),
            pltpu.VMEM((TILES, ROWS, LANES), BF16),
            pltpu.VMEM((TILES, ROWS, LANES), BF16),
            pltpu.VMEM((SLOT_TILES, RANKS, 2, LANES), BF16),
            pltpu.VMEM((SLOT_TILES, RANKS, 2, LANES), BF16),
            pltpu.VMEM((ROWS, LEAD), BF16),
            pltpu.SemaphoreType.DMA((len(inputs),)),
        ] + [pltpu.SemaphoreType.DMA((TILES + 1,))] * 2 + [
            pltpu.SemaphoreType.DMA((groups,))
        ] * 3 + [pltpu.SemaphoreType.REGULAR] * 2,
        compiler_params=pltpu.CompilerParams(
            collective_id=0, has_side_effects=True, vmem_limit_bytes=24 << 20
        ),
        cost_estimate=pl.CostEstimate(
            flops=60_000_000_000, bytes_accessed=4_000_000, transcendentals=0
        ),
    )(*inputs)
    step = 512
    result = pl.pallas_call(
        project,
        name="project",
        out_shape=jax.ShapeDtypeStruct((ROWS, OUT_WIDTH), BF16),
        in_specs=[vmem] * 5,
        out_specs=hbm,
        scratch_shapes=[
            pltpu.VMEM((OUT_WIDTH // step, ROWS, step), BF16),
            pltpu.SemaphoreType.DMA((OUT_WIDTH // step,)),
        ],
        compiler_params=pltpu.CompilerParams(vmem_limit_bytes=16 << 20),
        cost_estimate=pl.CostEstimate(
            flops=2 * ROWS * WIDTH * OUT_WIDTH, bytes_accessed=12_000_000, transcendentals=0
        ),
    )(packed, live, total, weight, proj_bias.reshape(1, OUT_WIDTH))
    return result[None]


def solution(mesh):
    placed = (
        P("enc", "grp", None, None),
        P("enc", "grp", None, None),
        P("enc", "grp"),
        P("enc", "grp"),
        P(),
        P(),
        P(),
        P(),
    )
    return jax.shard_map(
        shards, mesh=mesh, in_specs=placed, out_specs=P("enc", "grp", None), check_vma=False
    )
```

```python
import jax
import jax.numpy as jnp
from jax import lax
from jax.experimental import pallas as pl
from jax.experimental.pallas import tpu as pltpu
from jax.sharding import PartitionSpec as P

MESH = pl.DeviceIdType.MESH
F32 = jnp.float32
BF16 = jnp.bfloat16
LANES = 128
WIDTH = 1152
OUT_WIDTH = 4096
CLIPS = 64
PATCHES = 8
TOKENS = 3
RANKS = 64
ROWS = CLIPS * TOKENS
TILES = WIDTH // LANES
GROUPS = (
    ((6,), (), 0, 1),
    ((0, 3), (6, 0, 3), 1, 4),
    ((1, 4), (1, 4), 5, 3),
    ((2, 5), (2, 5), 8, 3),
    ((7,), (), 11, 1),
    ((8,), (7, 8), 12, 2),
)
PLACE = {tile: i for i, tile in enumerate(t for group in GROUPS for t in group[0])}
PAIR_AT = {tile: g[2] + i for g in GROUPS for i, tile in enumerate(g[0])}
THIRD_AT = {6: 3, 0: 4, 3: 4, 1: 7, 4: 7, 2: 10, 5: 10, 7: 13, 8: 13}
SLOT_TILES = 14
PIECE = 32
LEADING = 7
LEAD = LEADING * LANES


def iota(shape, dim):
    return lax.broadcasted_iota(jnp.int32, shape, dim)


def for_peers(me, act):
    x, y, core = me // 16, (me // 2) % 8, me % 2
    near = [
        ((x + dx) % 4) * 16 + (core + dcore) % 2 for dx in (2, 1, 3, 0) for dcore in (0, 1)
    ]

    def row(i, carry):
        dy = 4 + (1 - 2 * (i % 2)) * ((i + 1) // 2)
        at = ((y + dy) % 8) * 2
        for base in near:
            act(base + at)
        return carry

    lax.fori_loop(0, 7, row, 0)
    for i in (0, 1, 2, 3, 4, 5, 7):
        act(near[i] + 2 * y)


def exchange(
    feats_hbm, win_hbm, counts_hbm, owners_hbm, gain_hbm, bias_hbm, weight_hbm,
    packed_ref, live_ref, total_ref, weight_ref,
    feats, win_ref, counts_ref, owners_ref, gain_ref, bias_ref,
    stats, mine, theirs, outgoing, arrived, leading,
    fetch_sem, z_send, z_recv, x_send, x_recv, own_sem, column_sem, row_sem,
):
    me = lax.axis_index("grp")
    frame = lax.axis_index("enc")
    last = lax.axis_size("enc") - 1
    pairs = (
        (feats_hbm, feats), (win_hbm, win_ref), (counts_hbm, counts_ref),
        (owners_hbm, owners_ref), (gain_hbm, gain_ref), (bias_hbm, bias_ref),
        (weight_hbm, weight_ref),
    )
    fetches = [
        pltpu.make_async_copy(source, target, fetch_sem.at[i])
        for i, (source, target) in enumerate(pairs)
    ]
    for fetch in fetches[:-1]:
        fetch.start()

    barrier = pltpu.get_barrier_semaphore()
    before = jnp.maximum(frame - 1, 0)
    after = jnp.minimum(frame + 1, last)

    x, y, core = me // 16, (me // 2) % 8, me % 2
    column_peers = [16 * x + 2 * ((y + dy) % 8) + core for dy in (2, 6, 1, 7)]
    row_peers = [
        16 * ((x + dx) % 4) + 2 * y + (core + dcore) % 2
        for dx, dcore in ((2, 1), (2, 0), (1, 1), (3, 1), (1, 0), (3, 0), (0, 1))
    ]

    def tell(sem, peers):
        for peer in peers:
            pl.semaphore_signal(sem, inc=1, device_id={"grp": peer}, device_id_type=MESH)

    outer = frame > 0
    everyone = RANKS - 1

    def tell_plane(sem, condition):
        def signal(peer):
            @pl.when(peer != 0)
            def _():
                tell(sem, [peer])

        @pl.when(condition)
        def _():
            for_peers(me, signal)

    @pl.when(outer)
    def _():
        tell(barrier, column_peers + row_peers)

    @pl.when((frame == 0) & (me > 0))
    def _():
        tell(barrier, [0])

    @pl.when((frame == 0) & (me == 0))
    def _():
        tell(barrier, [1])

    tell_plane(barrier, (frame == 0) & (me > 0))

    @pl.when(frame > 0)
    def _():
        pl.semaphore_signal(barrier, inc=1, device_id={"enc": before}, device_id_type=MESH)

    @pl.when(frame < last)
    def _():
        pl.semaphore_signal(barrier, inc=1, device_id={"enc": after}, device_id_type=MESH)

    for fetch in fetches[:-1]:
        fetch.wait()
    fetches[-1].start()
    group = 32

    def statistics(i, carry):
        at = pl.ds(pl.multiple_of(i * group, group), group)
        values = feats[at, :].astype(F32)
        mean = jnp.sum(values, axis=1, keepdims=True) * (1.0 / WIDTH)
        centred = values - mean
        var = jnp.sum(centred * centred, axis=1, keepdims=True) * (1.0 / WIDTH)
        stats[0, at, :] = jnp.broadcast_to(mean, (group, LANES))
        stats[1, at, :] = jnp.broadcast_to(lax.rsqrt(var + 1e-6), (group, LANES))
        return carry

    lax.fori_loop(0, CLIPS * PATCHES // group, statistics, 0, unroll=2)
    diagonal = iota((LANES, LANES), 0) == iota((LANES, LANES), 1)

    def as_row(which, start):
        column = stats[which, pl.ds(start, LANES), :]
        return jnp.sum(jnp.where(diagonal, column, 0.0), axis=0, keepdims=True)

    half = CLIPS // 2
    depth = half * PATCHES
    clip_diagonal = iota((CLIPS, CLIPS), 0) == iota((CLIPS, CLIPS), 1)

    def pick_column(token, w):
        row = win_ref[token, w : w + 1, :]
        return jnp.sum(jnp.where(clip_diagonal, row, 0), axis=1, keepdims=True)

    picked = [
        [pick_column(token, w) + PATCHES * (iota((CLIPS, 1), 0) % half) for w in range(4)]
        for token in range(TOKENS)
    ]
    for block in range(2):
        start = block * depth
        mean_row = jnp.concatenate([as_row(0, start), as_row(0, start + LANES)], axis=1)
        rstd_row = jnp.concatenate([as_row(1, start), as_row(1, start + LANES)], axis=1)
        parts = []
        for token in range(TOKENS):
            lanes = iota((half, depth), 1)
            weight = jnp.zeros((half, depth), F32)
            for w in range(4):
                picks = picked[token][w][block * half : (block + 1) * half]
                weight += jnp.where(picks == lanes, 0.25, 0.0)
            parts.append(weight)
        scaled = jnp.concatenate(parts, axis=0) * rstd_row
        shift = jnp.sum(scaled * mean_row, axis=1, keepdims=True)
        high = scaled.astype(BF16)
        rest = scaled - high.astype(F32)
        middle = rest.astype(BF16)
        low = (rest - middle.astype(F32)).astype(BF16)
        selector = jnp.concatenate([high, middle, low], axis=0)
        height = TOKENS * half
        for column in range(0, WIDTH, 2 * LANES):
            wide = min(2 * LANES, WIDTH - column)
            product = jnp.dot(
                selector, feats[pl.ds(start, depth), pl.ds(column, wide)],
                preferred_element_type=F32,
            )
            total = product[:height] + product[height : 2 * height] + product[2 * height :]
            total = total - shift
            for i in range(wide // LANES):
                tile = column // LANES + i
                pooled = total[:, i * LANES : (i + 1) * LANES] * gain_ref[tile : tile + 1, :]
                pooled = (pooled + bias_ref[tile : tile + 1, :]).astype(BF16)
                for token in range(TOKENS):
                    at = pl.ds(token * CLIPS + block * half, half)
                    mine[PLACE[tile], at, :] = pooled[token * half : (token + 1) * half]

    @pl.when(frame == last)
    def _():
        theirs[...] = mine[...]

    owner_row = owners_ref[...]
    count_row = counts_ref[...].astype(F32)
    rank = iota((2 * RANKS, CLIPS), 0) // 2
    odd = iota((2 * RANKS, CLIPS), 0) % 2
    owned = jnp.where(owner_row == rank, 1.0, 0.0)
    even_rows = jnp.where(odd == 0, owned, 0.0)
    odd_rows = jnp.where(odd == 1, owned, 0.0)
    place_matrix = jnp.concatenate([even_rows, odd_rows], axis=1).astype(BF16)
    third_matrix = even_rows.astype(BF16)
    count_column = jnp.sum(odd_rows * count_row, axis=1, keepdims=True)

    neighbours = jnp.minimum(frame, 1) + jnp.minimum(last - frame, 1)
    late = (frame == 0) & (me > 1)
    greetings = jnp.where(
        outer, len(column_peers) + len(row_peers), jnp.where(late, everyone - 1, everyone)
    )
    pl.semaphore_wait(barrier, greetings + neighbours)

    @pl.when(outer)
    def _():
        tell(column_sem, column_peers)

    tell_plane(row_sem, (frame == 0) & (me == 1))

    pieces = ROWS // PIECE
    parts = [(0, 2 * CLIPS, 0), (0, CLIPS, TILES)] + [(p, ROWS, p) for p in range(1, TILES)]

    def shift(place, piece, sem):
        at = pl.ds(pl.multiple_of(piece * PIECE, PIECE), PIECE)
        pltpu.make_async_remote_copy(
            mine.at[place, at], theirs.at[place, at], z_send.at[sem], z_recv.at[sem],
            device_id={"enc": before}, device_id_type=MESH,
        ).start()

    @pl.when(frame > 0)
    def _():
        pairs_end = 2 * CLIPS // PIECE
        for piece in range(pieces):
            shift(0, piece, 0 if piece < pairs_end else TILES)

        def rest(i, carry):
            shift(i // pieces, i % pieces, i // pieces)
            return carry

        lax.fori_loop(pieces, TILES * pieces, rest, 0)

    @pl.when(outer)
    def _():
        pl.semaphore_wait(column_sem, len(column_peers))
        tell(row_sem, row_peers)
        pl.semaphore_wait(row_sem, len(row_peers))

    held = jnp.where(late, 0, -1)

    def shift_wait(part, sems):
        place, rows, sem = parts[part]
        at = pl.ds(0, rows)
        pltpu.make_async_copy(mine.at[place, at], theirs.at[place, at], sems.at[sem]).wait()

    def shifted(part):
        @pl.when(frame < last)
        def _():
            shift_wait(part, z_recv)

    def merge(place, at):
        return ((mine[place, at, :].astype(F32) + theirs[place, at, :].astype(F32)) * 0.5).astype(
            BF16
        )

    def lay_out(matrix, rows):
        return jnp.dot(matrix, rows, preferred_element_type=F32)

    def put(at, spread):
        outgoing[at] = spread.astype(BF16).reshape(RANKS, 2, LANES)

    def own_copy(i):
        at = pl.ds(*GROUPS[i][2:])
        return pltpu.make_async_copy(outgoing.at[at, me], arrived.at[at, me], own_sem.at[i])

    def send(i, peer):
        at = pl.ds(*GROUPS[i][2:])
        pltpu.make_async_remote_copy(
            outgoing.at[at, peer], arrived.at[at, me], x_send.at[i], x_recv.at[i],
            device_id={"grp": peer}, device_id_type=MESH,
        ).start()

    thirds_of = {}
    first_two, third_rows = pl.ds(0, 2 * CLIPS), pl.ds(2 * CLIPS, CLIPS)
    for i, (tiles, thirds, first, depth) in enumerate(GROUPS):
        for tile in tiles:
            place = PLACE[tile]
            shifted(place + 1 if place else 0)
            put(PAIR_AT[tile], lay_out(place_matrix, merge(place, first_two)))
            if place:
                thirds_of[tile] = merge(place, third_rows)
        if i == 1:
            shifted(1)
            put(THIRD_AT[6], lay_out(third_matrix, merge(0, third_rows)) + count_column)
        if thirds:
            rows = jnp.concatenate([thirds_of[tile] for tile in thirds[-2:]], axis=0)
            put(THIRD_AT[thirds[-1]], lay_out(place_matrix, rows))
        own_copy(i).start()

        def send_unheld(peer):
            @pl.when(peer != held)
            def _():
                send(i, peer)

        for_peers(me, send_unheld)

    @pl.when(late)
    def _():
        pl.semaphore_wait(row_sem, 1)
        for i in range(len(GROUPS)):
            send(i, 0)

    def arrival(i, sem):
        at = pl.ds(*GROUPS[i][2:])
        others = pl.ds(0, RANKS - 1)
        return pltpu.make_async_copy(outgoing.at[at, others], arrived.at[at, others], sem.at[i])

    def slot_tile(i):
        return arrived[i].reshape(2 * RANKS, LANES)

    for i, (tiles, thirds, first, depth) in enumerate(GROUPS):
        own_copy(i).wait()
        arrival(i, x_recv).wait()
        if i == 1:
            across = iota((2 * RANKS, 2 * RANKS), 1) // 2
            down = iota((2 * RANKS, 2 * RANKS), 0) // 2
            marked = iota((2 * RANKS, 2 * RANKS), 0) % 2 == 1
            earlier = jnp.where(marked & (down < across), 1.0, 0.0)
            same = jnp.where(marked & (down == across), 1.0, 0.0)
            table = jnp.concatenate([earlier, same], axis=1).astype(BF16)
            found = lax.dot_general(
                slot_tile(THIRD_AT[6]), table, (((0,), (0,)), ((), ())), preferred_element_type=F32
            )
            opening = found[:1, : 2 * RANKS].astype(jnp.int32)
            count = found[:1, 2 * RANKS :].astype(jnp.int32)
            row = iota((ROWS, 2 * RANKS), 0)
            token = iota((ROWS, 2 * RANKS), 1) % 2
            pair = (row == opening + token) & (token < count)
            third = (row == opening + 2) & (count == 3)
            pair = jnp.where(pair, 1.0, 0.0)
            third_even = jnp.where(third & (token == 0), 1.0, 0.0)
            third_odd = jnp.where(third & (token == 1), 1.0, 0.0)
            live = jnp.sum(pair + third_even, axis=1, keepdims=True)
            live_ref[...] = jnp.broadcast_to(live, (ROWS, LANES))
            pack = (
                jnp.concatenate([pair, third_even], axis=1).astype(BF16),
                jnp.concatenate([pair, third_odd], axis=1).astype(BF16),
            )
        for tile in thirds:
            side = tile in (3, 4, 5, 8)
            both = jnp.concatenate(
                [slot_tile(PAIR_AT[tile]), slot_tile(THIRD_AT[tile])], axis=0
            )
            packed = jnp.dot(pack[side], both, preferred_element_type=F32).astype(BF16)
            if tile < LEADING:
                leading[:, tile * LANES : (tile + 1) * LANES] = packed
            else:
                at = (tile - LEADING) * LANES
                packed_ref[:, at : at + LANES] = packed
        if i == 3:
            fetches[-1].wait()
            step = 512
            for column in range(0, OUT_WIDTH, step):
                at = pl.ds(column, step)
                total_ref[:, at] = jnp.dot(
                    leading[...], weight_ref[pl.ds(0, LEAD), at], preferred_element_type=F32
                )

    for i in range(len(GROUPS)):
        arrival(i, x_send).wait()

    @pl.when(frame > 0)
    def _():
        for part in range(len(parts)):
            shift_wait(part, z_send)


def project(packed_ref, live_ref, total_ref, weight_ref, bias_ref, result_ref, staged, sems):
    columns = staged.shape[2]
    shown = live_ref[:, :1] > 0.5

    def copy(n):
        at = pl.ds(n * columns, columns)
        return pltpu.make_async_copy(staged.at[n], result_ref.at[:, at], sems.at[n])

    for n in range(OUT_WIDTH // columns):
        at = pl.ds(n * columns, columns)
        product = total_ref[:, at] + jnp.dot(
            packed_ref[...], weight_ref[pl.ds(LEAD, WIDTH - LEAD), at],
            preferred_element_type=F32,
        )
        staged[n] = jnp.where(shown, product + bias_ref[:, at], 0.0).astype(BF16)
        copy(n).start()
    for n in range(OUT_WIDTH // columns):
        copy(n).wait()


def shards(patch_feats, windows, counts, owners, norm_gain, norm_bias, proj_weight, proj_bias):
    vmem = pl.BlockSpec(memory_space=pltpu.VMEM)
    hbm = pl.BlockSpec(memory_space=pltpu.HBM)
    groups = len(GROUPS)
    inputs = [
        pltpu.with_memory_space_constraint(array, pltpu.HBM)
        for array in (
            patch_feats.reshape(CLIPS * PATCHES, WIDTH), windows[0].transpose(1, 2, 0),
            counts, owners, norm_gain.reshape(TILES, LANES), norm_bias.reshape(TILES, LANES),
            proj_weight,
        )
    ]
    packed, live, total, weight = pl.pallas_call(
        exchange,
        name="exchange",
        out_shape=(
            jax.ShapeDtypeStruct((ROWS, WIDTH - LEAD), BF16),
            jax.ShapeDtypeStruct((ROWS, LANES), F32),
            jax.ShapeDtypeStruct((ROWS, OUT_WIDTH), F32),
            jax.ShapeDtypeStruct((WIDTH, OUT_WIDTH), BF16),
        ),
        in_specs=[hbm] * len(inputs),
        out_specs=(vmem,) * 4,
        scratch_shapes=[pltpu.VMEM(array.shape, array.dtype) for array in inputs[:-1]] + [
            pltpu.VMEM((2, CLIPS * PATCHES, LANES), F32),
            pltpu.VMEM((TILES, ROWS, LANES), BF16),
            pltpu.VMEM((TILES, ROWS, LANES), BF16),
            pltpu.VMEM((SLOT_TILES, RANKS, 2, LANES), BF16),
            pltpu.VMEM((SLOT_TILES, RANKS, 2, LANES), BF16),
            pltpu.VMEM((ROWS, LEAD), BF16),
            pltpu.SemaphoreType.DMA((len(inputs),)),
        ] + [pltpu.SemaphoreType.DMA((TILES + 1,))] * 2 + [
            pltpu.SemaphoreType.DMA((groups,))
        ] * 3 + [pltpu.SemaphoreType.REGULAR] * 2,
        compiler_params=pltpu.CompilerParams(
            collective_id=0, has_side_effects=True, vmem_limit_bytes=24 << 20
        ),
        cost_estimate=pl.CostEstimate(
            flops=60_000_000_000, bytes_accessed=4_000_000, transcendentals=0
        ),
    )(*inputs)
    step = 512
    result = pl.pallas_call(
        project,
        name="project",
        out_shape=jax.ShapeDtypeStruct((ROWS, OUT_WIDTH), BF16),
        in_specs=[vmem] * 5,
        out_specs=hbm,
        scratch_shapes=[
            pltpu.VMEM((OUT_WIDTH // step, ROWS, step), BF16),
            pltpu.SemaphoreType.DMA((OUT_WIDTH // step,)),
        ],
        compiler_params=pltpu.CompilerParams(vmem_limit_bytes=16 << 20),
        cost_estimate=pl.CostEstimate(
            flops=2 * ROWS * WIDTH * OUT_WIDTH, bytes_accessed=12_000_000, transcendentals=0
        ),
    )(packed, live, total, weight, proj_bias.reshape(1, OUT_WIDTH))
    return result[None]


def solution(mesh):
    placed = (
        P("enc", "grp", None, None),
        P("enc", "grp", None, None),
        P("enc", "grp"),
        P("enc", "grp"),
        P(),
        P(),
        P(),
        P(),
    )
    return jax.shard_map(
        shards, mesh=mesh, in_specs=placed, out_specs=P("enc", "grp", None), check_vma=False
    )
```

```python
import jax
import jax.numpy as jnp
from jax import lax
from jax.experimental import pallas as pl
from jax.experimental.pallas import tpu as pltpu
from jax.sharding import PartitionSpec as P

MESH = pl.DeviceIdType.MESH
F32 = jnp.float32
BF16 = jnp.bfloat16
LANES = 128
WIDTH = 1152
OUT_WIDTH = 4096
CLIPS = 64
PATCHES = 8
TOKENS = 3
RANKS = 64
ROWS = CLIPS * TOKENS
TILES = WIDTH // LANES
GROUPS = (
    ((6,), (6,), 0, 2),
    ((0, 3), (0, 3), 2, 3),
    ((1, 4), (1, 4), 5, 3),
    ((2, 5), (2, 5), 8, 3),
    ((7,), (), 11, 1),
    ((8,), (7, 8), 12, 2),
)
PLACE = {tile: i for i, tile in enumerate(t for group in GROUPS for t in group[0])}
PAIR_AT = {tile: g[2] + i for g in GROUPS for i, tile in enumerate(g[0])}
THIRD_AT = {6: 1, 0: 4, 3: 4, 1: 7, 4: 7, 2: 10, 5: 10, 7: 13, 8: 13}
SLOT_TILES = 14
PIECE = 32
LEADING = 7
LEAD = LEADING * LANES


def iota(shape, dim):
    return lax.broadcasted_iota(jnp.int32, shape, dim)


def for_peers(me, act):
    x, y, core = me // 16, (me // 2) % 8, me % 2
    near = [
        ((x + dx) % 4) * 16 + (core + dcore) % 2 for dx in (2, 1, 3, 0) for dcore in (0, 1)
    ]

    def row(i, carry):
        dy = 4 + (1 - 2 * (i % 2)) * ((i + 1) // 2)
        at = ((y + dy) % 8) * 2
        for base in near:
            act(base + at)
        return carry

    lax.fori_loop(0, 7, row, 0)
    for i in (0, 1, 2, 3, 4, 5, 7):
        act(near[i] + 2 * y)


def exchange(
    feats_hbm, win_hbm, counts_hbm, owners_hbm, gain_hbm, bias_hbm, weight_hbm,
    packed_ref, live_ref, total_ref, weight_ref,
    feats, win_ref, counts_ref, owners_ref, gain_ref, bias_ref,
    stats, mine, theirs, outgoing, arrived, leading,
    fetch_sem, z_send, z_recv, x_send, x_recv, own_sem, column_sem, row_sem,
):
    me = lax.axis_index("grp")
    frame = lax.axis_index("enc")
    last = lax.axis_size("enc") - 1
    quarter = pl.ds(0, CLIPS * PATCHES // 4)
    pairs = (
        (feats_hbm.at[quarter], feats.at[quarter]), (win_hbm, win_ref), (counts_hbm, counts_ref),
        (owners_hbm, owners_ref), (gain_hbm, gain_ref), (bias_hbm, bias_ref),
        (weight_hbm, weight_ref),
    )
    fetches = [
        pltpu.make_async_copy(source, target, fetch_sem.at[i])
        for i, (source, target) in enumerate(pairs)
    ]
    for i in range(1, 4):
        quarter = pl.ds(i * CLIPS * PATCHES // 4, CLIPS * PATCHES // 4)
        fetches.insert(
            i,
            pltpu.make_async_copy(
                feats_hbm.at[quarter], feats.at[quarter], fetch_sem.at[len(pairs) + i - 1]
            ),
        )
    for fetch in fetches[:-1]:
        fetch.start()

    barrier = pltpu.get_barrier_semaphore()
    before = jnp.maximum(frame - 1, 0)
    after = jnp.minimum(frame + 1, last)

    x, y, core = me // 16, (me // 2) % 8, me % 2
    column_peers = [16 * x + 2 * ((y + dy) % 8) + core for dy in (2, 6, 1, 7)]
    row_peers = [
        16 * ((x + dx) % 4) + 2 * y + (core + dcore) % 2
        for dx, dcore in ((2, 1), (2, 0), (1, 1), (3, 1), (1, 0), (3, 0), (0, 1))
    ]

    def tell(sem, peers):
        for peer in peers:
            pl.semaphore_signal(sem, inc=1, device_id={"grp": peer}, device_id_type=MESH)

    outer = frame > 0
    everyone = RANKS - 1

    def tell_plane(sem, condition):
        def signal(peer):
            @pl.when(peer != 0)
            def _():
                tell(sem, [peer])

        @pl.when(condition)
        def _():
            for_peers(me, signal)

    @pl.when(outer)
    def _():
        tell(barrier, column_peers + row_peers)

    @pl.when((frame == 0) & (me > 0))
    def _():
        tell(barrier, [0])

    @pl.when((frame == 0) & (me == 0))
    def _():
        tell(barrier, [1])

    tell_plane(barrier, (frame == 0) & (me > 0))

    @pl.when(frame > 0)
    def _():
        pl.semaphore_signal(barrier, inc=1, device_id={"enc": before}, device_id_type=MESH)

    @pl.when(frame < last)
    def _():
        pl.semaphore_signal(barrier, inc=1, device_id={"enc": after}, device_id_type=MESH)

    group = 32

    def statistics(i, carry):
        at = pl.ds(pl.multiple_of(i * group, group), group)
        values = feats[at, :].astype(F32)
        mean = jnp.sum(values, axis=1, keepdims=True) * (1.0 / WIDTH)
        centred = values - mean
        var = jnp.sum(centred * centred, axis=1, keepdims=True) * (1.0 / WIDTH)
        stats[0, at, :] = jnp.broadcast_to(mean, (group, LANES))
        stats[1, at, :] = jnp.broadcast_to(lax.rsqrt(var + 1e-6), (group, LANES))
        return carry

    steps = CLIPS * PATCHES // group // 4
    for i in range(4):
        fetches[i].wait()
        lax.fori_loop(i * steps, (i + 1) * steps, statistics, 0, unroll=2)
    fetches[-1].start()
    for fetch in fetches[4:-1]:
        fetch.wait()
    diagonal = iota((LANES, LANES), 0) == iota((LANES, LANES), 1)

    def as_row(which, start):
        column = stats[which, pl.ds(start, LANES), :]
        return jnp.sum(jnp.where(diagonal, column, 0.0), axis=0, keepdims=True)

    half = CLIPS // 2
    depth = half * PATCHES
    clip_diagonal = iota((CLIPS, CLIPS), 0) == iota((CLIPS, CLIPS), 1)

    def pick_column(token, w):
        row = win_ref[token, w : w + 1, :]
        return jnp.sum(jnp.where(clip_diagonal, row, 0), axis=1, keepdims=True)

    picked = [
        [pick_column(token, w) + PATCHES * (iota((CLIPS, 1), 0) % half) for w in range(4)]
        for token in range(TOKENS)
    ]
    for block in range(2):
        start = block * depth
        mean_row = jnp.concatenate([as_row(0, start), as_row(0, start + LANES)], axis=1)
        rstd_row = jnp.concatenate([as_row(1, start), as_row(1, start + LANES)], axis=1)
        parts = []
        for token in range(TOKENS):
            lanes = iota((half, depth), 1)
            weight = jnp.zeros((half, depth), F32)
            for w in range(4):
                picks = picked[token][w][block * half : (block + 1) * half]
                weight += jnp.where(picks == lanes, 0.25, 0.0)
            parts.append(weight)
        scaled = jnp.concatenate(parts, axis=0) * rstd_row
        shift = jnp.sum(scaled * mean_row, axis=1, keepdims=True)
        high = scaled.astype(BF16)
        rest = scaled - high.astype(F32)
        middle = rest.astype(BF16)
        low = (rest - middle.astype(F32)).astype(BF16)
        selector = jnp.concatenate([high, middle, low], axis=0)
        height = TOKENS * half
        for column in range(0, WIDTH, 2 * LANES):
            wide = min(2 * LANES, WIDTH - column)
            product = jnp.dot(
                selector, feats[pl.ds(start, depth), pl.ds(column, wide)],
                preferred_element_type=F32,
            )
            total = product[:height] + product[height : 2 * height] + product[2 * height :]
            total = total - shift
            for i in range(wide // LANES):
                tile = column // LANES + i
                pooled = total[:, i * LANES : (i + 1) * LANES] * gain_ref[tile : tile + 1, :]
                pooled = (pooled + bias_ref[tile : tile + 1, :]).astype(BF16)
                for token in range(TOKENS):
                    at = pl.ds(token * CLIPS + block * half, half)
                    mine[PLACE[tile], at, :] = pooled[token * half : (token + 1) * half]

    @pl.when(frame == last)
    def _():
        theirs[...] = mine[...]

    owner_row = owners_ref[...]
    count_row = counts_ref[...].astype(F32)
    rank = iota((2 * RANKS, CLIPS), 0) // 2
    odd = iota((2 * RANKS, CLIPS), 0) % 2
    owned = jnp.where(owner_row == rank, 1.0, 0.0)
    even_rows = jnp.where(odd == 0, owned, 0.0)
    odd_rows = jnp.where(odd == 1, owned, 0.0)
    place_matrix = jnp.concatenate([even_rows, odd_rows], axis=1).astype(BF16)
    third_matrix = even_rows.astype(BF16)
    count_column = jnp.sum(odd_rows * count_row, axis=1, keepdims=True)

    neighbours = jnp.minimum(frame, 1) + jnp.minimum(last - frame, 1)
    late = (frame == 0) & (me > 1)
    greetings = jnp.where(
        outer, len(column_peers) + len(row_peers), jnp.where(late, everyone - 1, everyone)
    )
    pl.semaphore_wait(barrier, greetings + neighbours)

    @pl.when(outer)
    def _():
        tell(column_sem, column_peers)

    tell_plane(row_sem, (frame == 0) & (me == 1))

    pieces = ROWS // PIECE

    @pl.when(frame > 0)
    def _():
        def shift(i, carry):
            place = i // pieces
            at = pl.ds(pl.multiple_of((i % pieces) * PIECE, PIECE), PIECE)
            pltpu.make_async_remote_copy(
                mine.at[place, at], theirs.at[place, at], z_send.at[place], z_recv.at[place],
                device_id={"enc": before}, device_id_type=MESH,
            ).start()
            return carry

        lax.fori_loop(0, TILES * pieces, shift, 0)

    @pl.when(outer)
    def _():
        pl.semaphore_wait(column_sem, len(column_peers))
        tell(row_sem, row_peers)

    held = jnp.where(late, 0, -1)

    def shift_wait(place, sems):
        pltpu.make_async_copy(mine.at[place], theirs.at[place], sems.at[place]).wait()

    def shifted(place):
        @pl.when(frame < last)
        def _():
            shift_wait(place, z_recv)

    def merge(place, at):
        return ((mine[place, at, :].astype(F32) + theirs[place, at, :].astype(F32)) * 0.5).astype(
            BF16
        )

    def lay_out(matrix, rows):
        return jnp.dot(matrix, rows, preferred_element_type=F32)

    def put(at, spread):
        outgoing[at] = spread.astype(BF16).reshape(RANKS, 2, LANES)

    def own_copy(i):
        at = pl.ds(*GROUPS[i][2:])
        return pltpu.make_async_copy(outgoing.at[at, me], arrived.at[at, me], own_sem.at[i])

    def send(i, peer):
        at = pl.ds(*GROUPS[i][2:])
        pltpu.make_async_remote_copy(
            outgoing.at[at, peer], arrived.at[at, me], x_send.at[i], x_recv.at[i],
            device_id={"grp": peer}, device_id_type=MESH,
        ).start()

    thirds_of = {}
    first_two, third_rows = pl.ds(0, 2 * CLIPS), pl.ds(2 * CLIPS, CLIPS)
    for i, (tiles, thirds, first, depth) in enumerate(GROUPS):
        for tile in tiles:
            place = PLACE[tile]
            shifted(place)
            put(PAIR_AT[tile], lay_out(place_matrix, merge(place, first_two)))
            thirds_of[tile] = merge(place, third_rows)
        if i == 0:
            put(THIRD_AT[6], lay_out(third_matrix, thirds_of[6]) + count_column)
        elif thirds:
            rows = jnp.concatenate([thirds_of[tile] for tile in thirds], axis=0)
            put(THIRD_AT[thirds[-1]], lay_out(place_matrix, rows))
        own_copy(i).start()
        if i == 0:
            @pl.when(outer)
            def _():
                pl.semaphore_wait(row_sem, len(row_peers))

        def send_unheld(peer):
            @pl.when(peer != held)
            def _():
                send(i, peer)

        for_peers(me, send_unheld)

    @pl.when(late)
    def _():
        pl.semaphore_wait(row_sem, 1)
        for i in range(len(GROUPS)):
            send(i, 0)

    def arrival(i, sem):
        at = pl.ds(*GROUPS[i][2:])
        others = pl.ds(0, RANKS - 1)
        return pltpu.make_async_copy(outgoing.at[at, others], arrived.at[at, others], sem.at[i])

    def slot_tile(i):
        return arrived[i].reshape(2 * RANKS, LANES)

    for i, (tiles, thirds, first, depth) in enumerate(GROUPS):
        own_copy(i).wait()
        arrival(i, x_recv).wait()
        if i == 0:
            across = iota((2 * RANKS, 2 * RANKS), 1) // 2
            down = iota((2 * RANKS, 2 * RANKS), 0) // 2
            marked = iota((2 * RANKS, 2 * RANKS), 0) % 2 == 1
            earlier = jnp.where(marked & (down < across), 1.0, 0.0)
            same = jnp.where(marked & (down == across), 1.0, 0.0)
            table = jnp.concatenate([earlier, same], axis=1).astype(BF16)
            found = lax.dot_general(
                slot_tile(THIRD_AT[6]), table, (((0,), (0,)), ((), ())), preferred_element_type=F32
            )
            opening = found[:1, : 2 * RANKS].astype(jnp.int32)
            count = found[:1, 2 * RANKS :].astype(jnp.int32)
            row = iota((ROWS, 2 * RANKS), 0)
            token = iota((ROWS, 2 * RANKS), 1) % 2
            pair = (row == opening + token) & (token < count)
            third = (row == opening + 2) & (count == 3)
            pair = jnp.where(pair, 1.0, 0.0)
            third_even = jnp.where(third & (token == 0), 1.0, 0.0)
            third_odd = jnp.where(third & (token == 1), 1.0, 0.0)
            live = jnp.sum(pair + third_even, axis=1, keepdims=True)
            live_ref[...] = jnp.broadcast_to(live, (ROWS, LANES))
            pack = (
                jnp.concatenate([pair, third_even], axis=1).astype(BF16),
                jnp.concatenate([pair, third_odd], axis=1).astype(BF16),
            )
        for tile in thirds:
            side = tile in (3, 4, 5, 8)
            both = jnp.concatenate(
                [slot_tile(PAIR_AT[tile]), slot_tile(THIRD_AT[tile])], axis=0
            )
            packed = jnp.dot(pack[side], both, preferred_element_type=F32).astype(BF16)
            if tile < LEADING:
                leading[:, tile * LANES : (tile + 1) * LANES] = packed
            else:
                at = (tile - LEADING) * LANES
                packed_ref[:, at : at + LANES] = packed
        if i == 3:
            fetches[-1].wait()
            step = 512
            for column in range(0, OUT_WIDTH, step):
                at = pl.ds(column, step)
                total_ref[:, at] = jnp.dot(
                    leading[...], weight_ref[pl.ds(0, LEAD), at], preferred_element_type=F32
                )

    for i in range(len(GROUPS)):
        arrival(i, x_send).wait()

    @pl.when(frame > 0)
    def _():
        for place in range(TILES):
            shift_wait(place, z_send)


def project(packed_ref, live_ref, total_ref, weight_ref, bias_ref, result_ref, staged, sems):
    columns = staged.shape[2]
    shown = live_ref[:, :1] > 0.5

    def copy(n):
        at = pl.ds(n * columns, columns)
        return pltpu.make_async_copy(staged.at[n], result_ref.at[:, at], sems.at[n])

    for n in range(OUT_WIDTH // columns):
        at = pl.ds(n * columns, columns)
        product = total_ref[:, at] + jnp.dot(
            packed_ref[...], weight_ref[pl.ds(LEAD, WIDTH - LEAD), at],
            preferred_element_type=F32,
        )
        staged[n] = jnp.where(shown, product + bias_ref[:, at], 0.0).astype(BF16)
        copy(n).start()
    for n in range(OUT_WIDTH // columns):
        copy(n).wait()


def shards(patch_feats, windows, counts, owners, norm_gain, norm_bias, proj_weight, proj_bias):
    vmem = pl.BlockSpec(memory_space=pltpu.VMEM)
    hbm = pl.BlockSpec(memory_space=pltpu.HBM)
    groups = len(GROUPS)
    inputs = [
        pltpu.with_memory_space_constraint(array, pltpu.HBM)
        for array in (
            patch_feats.reshape(CLIPS * PATCHES, WIDTH), windows[0].transpose(1, 2, 0),
            counts, owners, norm_gain.reshape(TILES, LANES), norm_bias.reshape(TILES, LANES),
            proj_weight,
        )
    ]
    packed, live, total, weight = pl.pallas_call(
        exchange,
        name="exchange",
        out_shape=(
            jax.ShapeDtypeStruct((ROWS, WIDTH - LEAD), BF16),
            jax.ShapeDtypeStruct((ROWS, LANES), F32),
            jax.ShapeDtypeStruct((ROWS, OUT_WIDTH), F32),
            jax.ShapeDtypeStruct((WIDTH, OUT_WIDTH), BF16),
        ),
        in_specs=[hbm] * len(inputs),
        out_specs=(vmem,) * 4,
        scratch_shapes=[pltpu.VMEM(array.shape, array.dtype) for array in inputs[:-1]] + [
            pltpu.VMEM((2, CLIPS * PATCHES, LANES), F32),
            pltpu.VMEM((TILES, ROWS, LANES), BF16),
            pltpu.VMEM((TILES, ROWS, LANES), BF16),
            pltpu.VMEM((SLOT_TILES, RANKS, 2, LANES), BF16),
            pltpu.VMEM((SLOT_TILES, RANKS, 2, LANES), BF16),
            pltpu.VMEM((ROWS, LEAD), BF16),
            pltpu.SemaphoreType.DMA((len(inputs) + 3,)),
        ] + [pltpu.SemaphoreType.DMA((TILES,))] * 2 + [
            pltpu.SemaphoreType.DMA((groups,))
        ] * 3 + [pltpu.SemaphoreType.REGULAR] * 2,
        compiler_params=pltpu.CompilerParams(
            collective_id=0, has_side_effects=True, vmem_limit_bytes=24 << 20
        ),
        cost_estimate=pl.CostEstimate(
            flops=60_000_000_000, bytes_accessed=4_000_000, transcendentals=0
        ),
    )(*inputs)
    step = 512
    result = pl.pallas_call(
        project,
        name="project",
        out_shape=jax.ShapeDtypeStruct((ROWS, OUT_WIDTH), BF16),
        in_specs=[vmem] * 5,
        out_specs=hbm,
        scratch_shapes=[
            pltpu.VMEM((OUT_WIDTH // step, ROWS, step), BF16),
            pltpu.SemaphoreType.DMA((OUT_WIDTH // step,)),
        ],
        compiler_params=pltpu.CompilerParams(vmem_limit_bytes=16 << 20),
        cost_estimate=pl.CostEstimate(
            flops=2 * ROWS * WIDTH * OUT_WIDTH, bytes_accessed=12_000_000, transcendentals=0
        ),
    )(packed, live, total, weight, proj_bias.reshape(1, OUT_WIDTH))
    return result[None]


def solution(mesh):
    placed = (
        P("enc", "grp", None, None),
        P("enc", "grp", None, None),
        P("enc", "grp"),
        P("enc", "grp"),
        P(),
        P(),
        P(),
        P(),
    )
    return jax.shard_map(
        shards, mesh=mesh, in_specs=placed, out_specs=P("enc", "grp", None), check_vma=False
    )
```
